32 devices in a mesh: path: 4 (over y, core), fsdp: 8 (over z, x).
Axes of the slice: x: 2, y: 2, z: 4, core: 2. Of those that a mesh axis runs over, the one named last changes fastest.
Arguments:
- input_activation_matrix: bfloat16 [4, 1536, 2048], P('path', 'fsdp'), may hold values from -6 to 6
- output_sensitivity: bfloat16 [4, 1536, 2048], P('path', 'fsdp'), may hold values from -12 to 12
- trajectory_initial_parameters: bfloat16 [4, 8, 1024, 4096], P('path', None, 'fsdp'), may hold values from -6 to 6
- trajectory_gradient_average: bfloat16 [4, 8, 1024, 4096], P('path', None, 'fsdp'), may hold values from -0.19921875 to 0.19921875
- trajectory_squared_average: bfloat16 [4, 8, 1024, 4096], P('path', None, 'fsdp'), may hold values from 0.0009994507 to 0.099609375
- common_expert_parameters: float32 [8, 2, 1024, 4096], P('path', None, 'fsdp'), may hold values from -6 to 6
- outer_inertia: float32 [8, 2, 1024, 4096], P('path', None, 'fsdp'), may hold values from -0.4 to 0.4
- trajectory_membership: int32 [4, 8], replicated, may hold values from 0 to 1
- punctual_flags: int32 [4], replicated, may hold values 0 or 1
Outputs:
- refreshed_experts: float32 [8, 2, 1024, 4096], P('path', None, 'fsdp')
- refreshed_inertia: float32 [8, 2, 1024, 4096], P('path', None, 'fsdp')
- returned: bfloat16 [4, 8, 1024, 4096], P('path', None, 'fsdp')
The draws below stay inside these ranges and needn't reach their ends.
All inputs are finite; a program needn't handle non-finite values.
Results may differ from the reference program's by a relative error of at most 0.0024.
Values may be sent and summed in bfloat16 or wider, within the bound.
A program may use at most 320 MiB of HBM per device.

```python
import math
import jax
import jax.numpy as jnp
from jax import lax

D = 2048
UNIT = 1024
SETS = 8
MPS = 2
STEP = 1000
TRAJECTORY_SUM = 4
TOKP = 1536


def touch_ends(array, own_key, smallest, largest):
    longest = array.shape.index(max(array.shape))
    spots = []
    for shift in (0, 1):
        where = [jax.random.randint(jax.random.fold_in(own_key, axis), (), 0, length) for axis, length in enumerate(array.shape)]
        where[longest] = (where[longest] + shift) % array.shape[longest]
        spots.append(tuple(where))
    return array.at[spots[0]].set(smallest).at[spots[1]].set(largest)


def block_levels(own_key, shape, pieces, smallest, largest):
    level = 1.0
    for position, parts in pieces:
        draws = jax.random.uniform(jax.random.fold_in(jax.random.fold_in(own_key, 6), position), (parts,), jnp.float32, smallest / len(pieces), largest / len(pieces))
        level = level * jnp.repeat(jnp.exp(draws), shape[position] // parts).reshape((-1,) + (1,) * (len(shape) - 1 - position))
    return level


def noise(key, shape, width, bound, shards=(), kind=jnp.bfloat16):
    level = block_levels(key, shape, shards, -0.22, 0.18) if shards else 1.0
    drawn = jax.random.normal(key, shape, jnp.float32) * width * level
    return jnp.minimum(jnp.maximum(drawn, -bound), bound).astype(kind)


def setup_inputs(seed: int = 0) -> dict:
    splits = jax.random.split(jax.random.key(seed), 10)
    input_activation_matrix = noise(splits[0], (TRAJECTORY_SUM, TOKP, D), 1.0, 6.0, ((0, 4), (1, 8)))
    output_sensitivity = noise(splits[1], (TRAJECTORY_SUM, TOKP, D), 2.0, 12.0, ((0, 4), (1, 8)))
    trajectory_initial_parameters = noise(splits[2], (TRAJECTORY_SUM, SETS, UNIT, 2 * D), 1.0, 6.0, ((0, 4), (2, 8)))
    trajectory_gradient_average = noise(splits[3], (TRAJECTORY_SUM, SETS, UNIT, 2 * D), 0.03, 0.19921875, ((0, 4), (2, 8)))
    trajectory_squared_average = jnp.clip(jnp.exp(math.log(0.099609375) - 4.6018058 * jax.random.uniform(splits[4], (TRAJECTORY_SUM, SETS, UNIT, 2 * D), jnp.float32) ** block_levels(splits[4], (TRAJECTORY_SUM, SETS, UNIT, 2 * D), ((0, 4), (2, 8)), -0.2, 0.2)), 0.0009994507, 0.099609375).astype(jnp.bfloat16)
    common_expert_parameters = noise(splits[5], (SETS, MPS, UNIT, 2 * D), 1.0, 6.0, ((0, 4), (2, 8)), jnp.float32)
    outer_inertia = noise(splits[6], (SETS, MPS, UNIT, 2 * D), 0.05, 0.4, ((0, 4), (2, 8)), jnp.float32)
    trajectory_membership = touch_ends(jax.random.randint(splits[7], (TRAJECTORY_SUM, SETS), 0, MPS), jax.random.fold_in(splits[7], 1), 0, MPS - 1).astype(jnp.int32)
    punctual_flags = touch_ends((jax.random.randint(splits[8], (TRAJECTORY_SUM,), 0, 2) < 1).astype(jnp.int32), jax.random.fold_in(splits[8], 1), 0, 1)
    return {"input_activation_matrix": input_activation_matrix, "output_sensitivity": output_sensitivity, "trajectory_initial_parameters": trajectory_initial_parameters, "trajectory_gradient_average": trajectory_gradient_average, "trajectory_squared_average": trajectory_squared_average, "common_expert_parameters": common_expert_parameters, "outer_inertia": outer_inertia, "trajectory_membership": trajectory_membership, "punctual_flags": punctual_flags}


BETA_ONE = 0.9
BETA_TWO = 0.999
ADAM_EPS = 1e-08
INNER_RATE = 0.05
DECAY = 0.1
GLOBAL_LEARNING = 0.7
INERTIA_FACTOR = 0.9

def adam_delta(grads, first, second, start):
    corr_one = 1.0 - BETA_ONE ** STEP
    corr_two = 1.0 - BETA_TWO ** STEP
    first_new = BETA_ONE * first.astype(jnp.float32) + (1.0 - BETA_ONE) * grads
    second_new = BETA_TWO * second.astype(jnp.float32) + (1.0 - BETA_TWO) * grads * grads
    direction = first_new / corr_one / (jnp.sqrt(second_new / corr_two) + ADAM_EPS)
    return (INNER_RATE * (direction + DECAY * start.astype(jnp.float32))).astype(jnp.bfloat16)

def path_grads(unit_rows, inputs, upstream):
    features = inputs.shape[1]
    in_rows = unit_rows[:, :features]
    out_rows = unit_rows[:, features:]
    input_scale = features ** (-0.5)
    hidden_scale = (SETS * UNIT) ** (-0.5)
    preact = jnp.dot(inputs, in_rows.T, preferred_element_type=jnp.float32) * input_scale
    active, pullback = jax.vjp(jax.nn.gelu, preact)
    active_half = active.astype(jnp.bfloat16)
    back_active = jnp.dot(upstream, out_rows.T, preferred_element_type=jnp.float32) * hidden_scale
    back_preact = pullback(back_active)[0].astype(jnp.bfloat16)
    grad_in = jnp.dot(back_preact.T, inputs, preferred_element_type=jnp.float32) * input_scale
    grad_out = jnp.dot(active_half.T, upstream, preferred_element_type=jnp.float32) * hidden_scale
    return jnp.concatenate([grad_in, grad_out], axis=1)

def reference(input_activation_matrix, output_sensitivity, trajectory_initial_parameters, trajectory_gradient_average, trajectory_squared_average, common_expert_parameters, outer_inertia, trajectory_membership, punctual_flags):
    eligible_trajectories = jnp.arange(MPS, dtype=jnp.int32)
    picked_trajectories = jnp.where((trajectory_membership[:, :, None] == eligible_trajectories[None, None, :]) & (punctual_flags[:, None, None] == 1), 1.0, 0.0).astype(jnp.float32)

    def accumulate(aggregate_change, items):
        inputs, upstream, start, first, second, weights = items
        unit_rows = start.reshape(SETS * UNIT, 2 * D)
        grads = path_grads(unit_rows, inputs, upstream)
        pseudo = adam_delta(grads, first.reshape(SETS * UNIT, 2 * D), second.reshape(SETS * UNIT, 2 * D), unit_rows)
        pseudo = pseudo.reshape(SETS, UNIT, 2 * D)
        return (aggregate_change + weights[:, :, None, None] * pseudo.astype(jnp.float32)[:, None], None)
    initial = jnp.zeros((SETS, MPS, UNIT, 2 * D), jnp.float32)
    aggregate_change, _ = lax.scan(accumulate, initial, (input_activation_matrix, output_sensitivity, trajectory_initial_parameters, trajectory_gradient_average, trajectory_squared_average, picked_trajectories))
    punctual_tally = lax.optimization_barrier(jnp.sum(picked_trajectories, axis=0))
    punctual_average = aggregate_change / jnp.maximum(punctual_tally, 1.0)[:, :, None, None]
    refreshed_inertia = INERTIA_FACTOR * outer_inertia + punctual_average
    refreshed_experts = common_expert_parameters - GLOBAL_LEARNING * (punctual_average + INERTIA_FACTOR * refreshed_inertia)
    updated = refreshed_experts.astype(jnp.bfloat16)
    set_index = jnp.arange(SETS, dtype=jnp.int32)
    returned = updated[set_index[None, :], trajectory_membership]
    return (refreshed_experts, refreshed_inertia, returned)
```

```python
import functools

import jax
import jax.numpy as jnp
from jax import lax
from jax.experimental import pallas as pl
from jax.experimental.pallas import tpu as pltpu
from jax.sharding import PartitionSpec as P

UNIT = 1024
SETS = 8
STEP = 1000


BETA_ONE = 0.9
BETA_TWO = 0.999
ADAM_EPS = 1e-08
INNER_RATE = 0.05
DECAY = 0.1
GLOBAL_LEARNING = 0.7
INERTIA_FACTOR = 0.9

MESH = pl.DeviceIdType.MESH
GELU_ROOT = 0.7978845608028654
GELU_CUBE = 0.044715


def adam_delta(grads, first, second, start):
    corr_one = 1.0 - BETA_ONE**STEP
    corr_two = 1.0 - BETA_TWO**STEP
    first_new = BETA_ONE * first.astype(jnp.float32) + (1.0 - BETA_ONE) * grads
    second_new = BETA_TWO * second.astype(jnp.float32) + (1.0 - BETA_TWO) * grads * grads
    direction = first_new / corr_one / (jnp.sqrt(second_new / corr_two) + ADAM_EPS)
    return (INNER_RATE * (direction + DECAY * start.astype(jnp.float32))).astype(jnp.bfloat16)


def gelu_pair(pre):
    square = pre * pre
    tanh = jnp.tanh(GELU_ROOT * pre * (1.0 + GELU_CUBE * square))
    half = 0.5 * (1.0 + tanh)
    slope = half + 0.5 * pre * (1.0 - tanh * tanh) * GELU_ROOT * (1.0 + 3.0 * GELU_CUBE * square)
    return pre * half, slope


def divisor(total, wanted):
    size = min(total, wanted)
    while total % size:
        size //= 2
    return size


class Plan:
    def __init__(self, paths, ring, shard, features, rows):
        self.paths, self.ring, self.shard = paths, ring, shard
        self.features, self.width, self.rows = features, 2 * features, rows
        self.tokens = ring * shard
        self.half = shard // 2
        self.owned = rows // paths
        self.group = 1
        while (self.group * shard) % 128:
            self.group *= 2
        self.batch = self.group * shard
        self.tile = divisor(features, 512)
        self.tiles = self.width // self.tile
        self.units = divisor(rows, 256)


def ring_neighbours(index, size):
    odd = index % 2
    rank = (1 - odd) * (index // 2) + odd * (size - (index + 1) // 2)

    def place(r):
        high = r // (size // 2)
        return (1 - high) * 2 * r + high * (2 * (size - r) - 1)

    return place((rank + 1) % size), place((rank + size - 1) % size)


def path_kernel(
    plan, single, active_ref, x_hbm, g_hbm, r_hbm, m_hbm, v_hbm, arr_hbm, own_hbm, *scratch
):
    (xg, params, hidden, first, second, pseudo) = scratch[:6]
    if single:
        (raw, swapped, cross_in, own_in, cross_out, own_out) = scratch[6:12]
    (load_sem, moment_sem, send_sem, recv_sem, side_send, side_recv, out_send, out_recv, keep_sem) = (
        scratch[-9:]
    )
    n, shard, half = plan.ring, plan.shard, plan.half
    features, owned, tile, tiles = plan.features, plan.owned, plan.tile, plan.tiles
    path = lax.axis_index("path")
    place = lax.axis_index("fsdp")
    ahead, behind = ring_neighbours(place, n)
    core = path % 2
    sibling = path + 1 - 2 * core
    lanes = 1 if single else 2

    barrier = pltpu.get_barrier_semaphore()
    for spot in (ahead, behind):
        pl.semaphore_signal(
            barrier, inc=1, device_id={"path": path, "fsdp": spot}, device_id_type=MESH
        )
    for k in range(1, plan.paths):
        pl.semaphore_signal(
            barrier,
            inc=1,
            device_id={"path": (path + k) % plan.paths, "fsdp": place},
            device_id_type=MESH,
        )

    def moments(t, slot):
        cols = pl.ds(pl.multiple_of(t * tile, tile), tile)
        return (
            pltpu.make_async_copy(m_hbm.at[:, cols], first.at[slot], moment_sem.at[0, slot]),
            pltpu.make_async_copy(v_hbm.at[:, cols], second.at[slot], moment_sem.at[1, slot]),
        )

    if single:
        loads = (
            pltpu.make_async_copy(x_hbm, raw.at[0], load_sem.at[0]),
            pltpu.make_async_copy(g_hbm, raw.at[1], load_sem.at[1]),
        )
    else:
        loads = (
            pltpu.make_async_copy(x_hbm, xg.at[0, pl.ds(0, shard)], load_sem.at[0]),
            pltpu.make_async_copy(g_hbm, xg.at[1, pl.ds(0, shard)], load_sem.at[1]),
        )
    for load in loads:
        load.start()
    load_params = pltpu.make_async_copy(r_hbm, params, load_sem.at[2])
    load_params.start()
    for load in moments(0, 0):
        load.start()
    pl.semaphore_wait(barrier, plan.paths + 1)
    for load in loads:
        load.wait()

    def ring_copy(step, lane, way):
        array = core if single else lane
        source = pl.ds(pl.multiple_of((step - 1) * shard + way * half, half), half)
        target = pl.ds(pl.multiple_of(step * shard + way * half, half), half)
        return pltpu.make_async_remote_copy(
            src_ref=xg.at[array, source],
            dst_ref=xg.at[array, target],
            send_sem=send_sem.at[lane, way, step],
            recv_sem=recv_sem.at[lane, way, step],
            device_id={"path": path, "fsdp": behind if way else ahead},
            device_id_type=MESH,
        )

    def side_copy(slot, array):
        rows = pl.ds(pl.multiple_of(slot * shard, shard), shard)
        return pltpu.make_async_remote_copy(
            src_ref=xg.at[array, rows],
            dst_ref=xg.at[array, rows],
            send_sem=side_send.at[slot],
            recv_sem=side_recv.at[slot],
            device_id={"path": sibling, "fsdp": place},
            device_id_type=MESH,
        )

    if single:
        active = active_ref[0] == core
        swap = pltpu.make_async_remote_copy(
            src_ref=raw.at[1 - core],
            dst_ref=swapped,
            send_sem=load_sem.at[3],
            recv_sem=load_sem.at[4],
            device_id={"path": sibling, "fsdp": place},
            device_id_type=MESH,
        )
        swap.start()
        swap.wait()
        xg[core, 0:shard] = jnp.where(active, raw[core], swapped[...])

    load_params.wait()

    def forward(j):
        rows = pl.ds(pl.multiple_of(j * plan.batch, plan.batch), plan.batch)

        def unit(u, carry):
            strip = pl.ds(pl.multiple_of(u * plan.units, plan.units), plan.units)
            nt = (((1,), (1,)), ((), ()))
            pre = lax.dot_general(
                params[strip, 0:features], xg[0, rows], nt, preferred_element_type=jnp.float32
            ) * (features**-0.5)
            act, slope = gelu_pair(pre)
            hidden[1, strip, rows] = act.astype(jnp.bfloat16)
            back = lax.dot_general(
                params[strip, features : 2 * features],
                xg[1, rows],
                nt,
                preferred_element_type=jnp.float32,
            ) * ((SETS * UNIT) ** -0.5)
            hidden[0, strip, rows] = (back * slope).astype(jnp.bfloat16)
            return carry

        lax.fori_loop(0, plan.rows // plan.units, unit, 0)

    def gather_batch(j, carry):
        for i in range(plan.group):
            k = j * plan.group + i

            @pl.when(k > 0)
            def _():
                for lane in range(lanes):
                    for way in range(2):
                        ring_copy(k, lane, way).wait_recv()

            @pl.when(k < n - 1)
            def _():
                for lane in range(lanes):
                    for way in range(2):
                        ring_copy(k + 1, lane, way).start()

            if single:
                side_copy(k, core).start()
        if single:
            for i in range(plan.group):
                side_copy(j * plan.group + i, 1 - core).wait_recv()
        forward(j)
        return carry

    lax.fori_loop(0, n // plan.group, gather_batch, 0)

    def cols_of(t):
        return pl.ds(pl.multiple_of(t * tile, tile), tile)

    def rows_of(p):
        return pl.ds(pl.multiple_of(p * owned, owned), owned)

    chip = path // 2
    far = (1 - chip) * 2

    def out_copy(t, k):
        owner = (path + k) % plan.paths
        return pltpu.make_async_remote_copy(
            src_ref=pseudo.at[rows_of(owner), cols_of(t)],
            dst_ref=arr_hbm.at[path, :, cols_of(t)],
            send_sem=out_send.at[t, k],
            recv_sem=out_recv.at[t, k],
            device_id={"path": owner, "fsdp": place},
            device_id_type=MESH,
        )

    def keep_copy(t):
        return pltpu.make_async_copy(
            pseudo.at[rows_of(path), cols_of(t)],
            arr_hbm.at[path, :, cols_of(t)],
            keep_sem.at[0, t],
        )

    def share_copy(t, which):
        owner = (far + 1 - core) if which == 0 else sibling
        return pltpu.make_async_remote_copy(
            src_ref=pseudo.at[rows_of(owner), cols_of(t)],
            dst_ref=(cross_in if which == 0 else own_in).at[t],
            send_sem=out_send.at[t, which],
            recv_sem=out_recv.at[t, which],
            device_id={"path": sibling, "fsdp": place},
            device_id_type=MESH,
        )

    def cross_copy(t):
        return pltpu.make_async_remote_copy(
            src_ref=cross_out.at[t],
            dst_ref=arr_hbm.at[chip, :, cols_of(t)],
            send_sem=out_send.at[t, 2],
            recv_sem=out_recv.at[t, 2],
            device_id={"path": far + core, "fsdp": place},
            device_id_type=MESH,
        )

    def near_copy(t):
        return pltpu.make_async_copy(
            own_out.at[t], arr_hbm.at[chip, :, cols_of(t)], keep_sem.at[0, t]
        )

    def late_copy(t):
        return pltpu.make_async_copy(
            pseudo.at[pl.ds(pl.multiple_of(far * owned, 2 * owned), 2 * owned), cols_of(t)],
            own_hbm.at[:, cols_of(t)],
            keep_sem.at[1, t],
        )

    def pick(t):
        share_copy(t, 0).wait_recv()
        cross_out[t] = jnp.where(active, pseudo[rows_of(far + core), cols_of(t)], cross_in[t])
        cross_copy(t).start()
        share_copy(t, 1).wait_recv()
        own_out[t] = jnp.where(active, pseudo[rows_of(path), cols_of(t)], own_in[t])
        near_copy(t).start()

    def grad_tile(t, carry):
        slot = t % 2

        @pl.when(t + 1 < tiles)
        def _():
            for load in moments(t + 1, 1 - slot):
                load.start()

        for load in moments(t, slot):
            load.wait()
        side = t // (tiles // 2)
        scale = jnp.where(side == 0, features**-0.5, (SETS * UNIT) ** -0.5).astype(jnp.float32)
        token_cols = pl.ds(pl.multiple_of(t % (tiles // 2) * tile, tile), tile)

        def unit(u, inner):
            strip = pl.ds(pl.multiple_of(u * plan.units, plan.units), plan.units)
            grads = (
                jnp.dot(
                    hidden[side, strip, :],
                    xg[side, :, token_cols],
                    preferred_element_type=jnp.float32,
                )
                * scale
            )
            pseudo[strip, cols_of(t)] = adam_delta(
                grads, first[slot, strip, :], second[slot, strip, :], params[strip, cols_of(t)]
            )
            return inner

        lax.fori_loop(0, plan.rows // plan.units, unit, 0)
        if single:
            share_copy(t, 0).start()
            share_copy(t, 1).start()
            late_copy(t).start()

            @pl.when(t > 0)
            def _():
                pick(t - 1)
        else:
            for k in range(plan.paths - 1, 0, -1):
                out_copy(t, k).start()
            keep_copy(t).start()
        return carry

    lax.fori_loop(0, tiles, grad_tile, 0)
    if single:
        pick(tiles - 1)

    def drain_ring(k, carry):
        for lane in range(lanes):
            for way in range(2):
                ring_copy(k, lane, way).wait_send()
        return carry

    lax.fori_loop(1, n, drain_ring, 0)
    if single:

        def drain_side(k, carry):
            side_copy(k, core).wait_send()
            return carry

        lax.fori_loop(0, n, drain_side, 0)

    def drain(t, carry):
        if single:
            share_copy(t, 0).wait_send()
            share_copy(t, 1).wait_send()
            late_copy(t).wait()
            near_copy(t).wait()
            cross_copy(t).wait()
        else:
            for k in range(1, plan.paths):
                out_copy(t, k).wait()
            keep_copy(t).wait()
        return carry

    lax.fori_loop(0, tiles, drain, 0)


def run_path(plan, single, active, x, g, r, m, v):
    bf16 = jnp.bfloat16
    width, tile, tiles = plan.width, plan.tile, plan.tiles
    scratch = [
        pltpu.VMEM((2, plan.tokens, plan.features), bf16),
        pltpu.VMEM((plan.rows, width), bf16),
        pltpu.VMEM((2, plan.rows, plan.tokens), bf16),
        pltpu.VMEM((2, plan.rows, tile), bf16),
        pltpu.VMEM((2, plan.rows, tile), bf16),
        pltpu.VMEM((plan.rows, width), bf16),
    ]
    if single:
        scratch += [
            pltpu.VMEM((2, plan.shard, plan.features), bf16),
            pltpu.VMEM((plan.shard, plan.features), bf16),
        ] + [pltpu.VMEM((tiles, plan.owned, tile), bf16)] * 4
    lanes = 1 if single else 2
    outs = 3 if single else plan.paths
    dma = pltpu.SemaphoreType.DMA
    scratch += [
        dma((5,)),
        dma((2, 2)),
        dma((lanes, 2, plan.ring)),
        dma((lanes, 2, plan.ring)),
        dma((plan.ring,)),
        dma((plan.ring,)),
        dma((tiles, outs)),
        dma((tiles, outs)),
        dma((2, tiles)),
    ]
    sources = 2 if single else plan.paths
    flops = 8 * plan.tokens * plan.features * plan.rows
    shapes = [jax.ShapeDtypeStruct((sources, plan.owned, width), bf16)]
    if single:
        shapes.append(jax.ShapeDtypeStruct((2 * plan.owned, width), bf16))
    body = functools.partial(path_kernel, plan, single)
    if not single:
        inner = body

        def body(active_ref, x, g, r, m, v, arr, *rest):
            inner(active_ref, x, g, r, m, v, arr, None, *rest)

    anywhere = pl.BlockSpec(memory_space=pl.ANY)
    return pl.pallas_call(
        body,
        out_shape=shapes,
        in_specs=[pl.BlockSpec(memory_space=pltpu.SMEM)] + [anywhere] * 5,
        out_specs=[anywhere] * len(shapes),
        scratch_shapes=scratch,
        compiler_params=pltpu.CompilerParams(
            collective_id=0 if single else 1,
            has_side_effects=True,
            vmem_limit_bytes=63 * 1024 * 1024,
        ),
        cost_estimate=pl.CostEstimate(
            flops=flops, bytes_accessed=8 * plan.rows * width, transcendentals=0
        ),
        name="single_path" if single else "both_paths",
    )(active, x, g, r, m, v)


def refresh(total, tally, common, inertia):
    average = total / tally
    inertia = INERTIA_FACTOR * inertia + average
    expert = common - GLOBAL_LEARNING * (average + INERTIA_FACTOR * inertia)
    return expert, inertia


def per_device(
    input_activation_matrix,
    output_sensitivity,
    trajectory_initial_parameters,
    trajectory_gradient_average,
    trajectory_squared_average,
    common_expert_parameters,
    outer_inertia,
    trajectory_membership,
    punctual_flags,
):
    set_count, local_units, row_width = trajectory_initial_parameters.shape[1:]
    rows = set_count * local_units
    path_count = lax.axis_size("path")
    position = lax.axis_index("path")
    owned_sets = set_count // path_count
    choices = common_expert_parameters.shape[1]
    plan = Plan(
        path_count,
        lax.axis_size("fsdp"),
        input_activation_matrix.shape[1],
        row_width // 2,
        rows,
    )
    x, g = input_activation_matrix[0], output_sensitivity[0]
    r, m, v = (
        array[0].reshape(rows, row_width)
        for array in (
            trajectory_initial_parameters,
            trajectory_gradient_average,
            trajectory_squared_average,
        )
    )
    member, flags = trajectory_membership, punctual_flags == 1
    picked = jnp.where(
        (member[:, :, None] == jnp.arange(choices, dtype=jnp.int32)) & flags[:, None, None],
        1.0,
        0.0,
    ).astype(jnp.float32)
    first_set = position * owned_sets
    tally = jnp.maximum(
        lax.dynamic_slice_in_dim(jnp.sum(picked, axis=0), first_set, owned_sets, 0), 1.0
    )
    wide = (slice(None), None, None)

    def choose(options, index):
        chosen = options[0]
        for c in range(1, choices):
            chosen = jnp.where(index == c, options[c], chosen)
        return chosen

    def put(returned, block, at):
        return lax.dynamic_update_slice(returned, block[None, None], (0, at, 0, 0))

    empty = jnp.zeros((1, set_count, local_units, row_width), jnp.bfloat16)

    def both():
        (arrived,) = run_path(plan, False, jnp.zeros((1,), jnp.int32), x, g, r, m, v)
        weights = lax.dynamic_slice_in_dim(picked, first_set, owned_sets, 1)
        hops = list(range(path_count - 1, 0, -1))
        trade = {k: [(p, p ^ k) for p in range(path_count)] for k in hops}
        experts, inertias = [], []
        returned = empty
        for j in range(owned_sets):
            part = slice(j * local_units, (j + 1) * local_units)
            total = sum(
                weights[p, j][wide] * arrived[p, part].astype(jnp.float32)[None]
                for p in range(path_count)
            )
            expert, inertia = refresh(
                total, tally[j][wide], common_expert_parameters[j], outer_inertia[j]
            )
            experts.append(expert)
            inertias.append(inertia)
            updated = expert.astype(jnp.bfloat16)
            for k in hops + [0]:
                chosen = choose(updated, member[position ^ k, first_set + j])
                if k:
                    chosen = lax.ppermute(chosen, "path", trade[k])
                returned = put(returned, chosen, (position ^ k) * owned_sets + j)
        return jnp.stack(experts), jnp.stack(inertias), returned

    def single():
        chip, core = position // 2, position % 2
        sibling, far = position ^ 1, (1 - chip) * 2
        cross = [(p, p ^ 2) for p in range(path_count)]
        swap = [(p, p ^ 1) for p in range(path_count)]
        alive = flags.reshape(2, 2)
        lead = jnp.where(alive[:, 1], 1, 0)
        leads = jnp.arange(2) * 2 + lead
        any_alive = jnp.any(alive, axis=1)
        lead_member = member[leads]
        owner_chip = jnp.arange(set_count) // (2 * owned_sets)
        same = jnp.where(owner_chip == 0, member[2] == member[3], member[0] == member[1])
        shared = jnp.where(owner_chip == 0, member[2], member[0])
        near = jnp.where(owner_chip == 0, lead_member[0], lead_member[1])
        late = jnp.where(same, shared, near)

        still = []
        for j in range(owned_sets):
            index = 1 - late[first_set + j]
            base, _ = refresh(
                jnp.float32(0.0),
                jnp.float32(1.0),
                choose(common_expert_parameters[j], index),
                choose(outer_inertia[j], index),
            )
            sent = lax.ppermute(base.astype(jnp.bfloat16), "path", cross)
            still.append((sent, lax.ppermute(sent, "path", swap)))

        arrived, mine = run_path(plan, True, lead[chip][None], x, g, r, m, v)

        experts, inertias, moved = [], [], []
        returned = empty
        for j in range(owned_sets):
            at = first_set + j
            part = slice(j * local_units, (j + 1) * local_units)
            total = sum(
                jnp.where(any_alive[c] & (lead_member[c, at] == jnp.arange(choices)), 1.0, 0.0)[wide]
                * arrived[c, part].astype(jnp.float32)[None]
                for c in range(2)
            )
            expert, inertia = refresh(
                total, tally[j][wide], common_expert_parameters[j], outer_inertia[j]
            )
            experts.append(expert)
            inertias.append(inertia)
            updated = expert.astype(jnp.bfloat16)
            sent = lax.ppermute(choose(updated, late[at]), "path", cross)
            moved.append((sent, lax.ppermute(sent, "path", swap)))
            returned = put(returned, choose(updated, member[position, at]), at)
            beside = lax.ppermute(choose(updated, member[sibling, at]), "path", swap)
            returned = put(returned, beside, sibling * owned_sets + j)
        gain = jnp.where(flags[position], GLOBAL_LEARNING * (1.0 + INERTIA_FACTOR), 0.0)
        for j in range(owned_sets):
            for turn in range(2):
                serving = core ^ turn
                at = (far + serving) * owned_sets + j
                share = lax.dynamic_slice_in_dim(
                    mine, (serving * owned_sets + j) * local_units, local_units, 0
                )
                quiet = still[j][turn].astype(jnp.float32) - gain * share.astype(jnp.float32)
                block = jnp.where(
                    member[position, at] == late[at], moved[j][turn], quiet.astype(jnp.bfloat16)
                )
                returned = put(returned, block, at)
        return jnp.stack(experts), jnp.stack(inertias), returned

    if path_count == 4 and choices == 2:
        lone = jnp.all(jnp.sum(flags.reshape(2, 2).astype(jnp.int32), axis=1) <= 1)
        return lax.cond(lone, single, both)
    return both()


def solution(mesh):
    placed = (
        P("path", "fsdp", None),
        P("path", "fsdp", None),
        P("path", None, "fsdp", None),
        P("path", None, "fsdp", None),
        P("path", None, "fsdp", None),
        P("path", None, "fsdp", None),
        P("path", None, "fsdp", None),
        P(),
        P(),
    )
    return jax.shard_map(
        per_device,
        mesh=mesh,
        in_specs=placed,
        out_specs=(
            P("path", None, "fsdp", None),
            P("path", None, "fsdp", None),
            P("path", None, "fsdp", None),
        ),
        check_vma=False,
    )
```

```python
import functools

import jax
import jax.numpy as jnp
from jax import lax
from jax.experimental import pallas as pl
from jax.experimental.pallas import tpu as pltpu
from jax.sharding import PartitionSpec as P


UNIT = 1024
SETS = 8
STEP = 1000


BETA_ONE = 0.9
BETA_TWO = 0.999
ADAM_EPS = 1e-08
INNER_RATE = 0.05
DECAY = 0.1
GLOBAL_LEARNING = 0.7
INERTIA_FACTOR = 0.9

MESH = pl.DeviceIdType.MESH
GELU_ROOT = 0.7978845608028654
GELU_CUBE = 0.044715


def adam_delta(grads, first, second, start):
    corr_one = 1.0 - BETA_ONE**STEP
    corr_two = 1.0 - BETA_TWO**STEP
    first_new = BETA_ONE * first.astype(jnp.float32) + (1.0 - BETA_ONE) * grads
    second_new = BETA_TWO * second.astype(jnp.float32) + (1.0 - BETA_TWO) * grads * grads
    direction = first_new / corr_one / (jnp.sqrt(second_new / corr_two) + ADAM_EPS)
    return (INNER_RATE * (direction + DECAY * start.astype(jnp.float32))).astype(jnp.bfloat16)


def gelu_pair(pre):
    square = pre * pre
    tanh = jnp.tanh(GELU_ROOT * pre * (1.0 + GELU_CUBE * square))
    half = 0.5 * (1.0 + tanh)
    slope = half + 0.5 * pre * (1.0 - tanh * tanh) * GELU_ROOT * (1.0 + 3.0 * GELU_CUBE * square)
    return pre * half, slope


def divisor(total, wanted):
    size = min(total, wanted)
    while total % size:
        size //= 2
    return size


class Plan:
    def __init__(self, paths, ring, shard, features, rows):
        self.paths, self.ring, self.shard = paths, ring, shard
        self.features, self.width, self.rows = features, 2 * features, rows
        self.tokens = ring * shard
        self.half = shard // 2
        self.owned = rows // paths
        self.group = 1
        while (self.group * shard) % 128:
            self.group *= 2
        self.batch = self.group * shard
        self.tile = divisor(features, 512)
        self.tiles = self.width // self.tile
        self.units = divisor(rows, 256)


def ring_neighbours(index, size):
    odd = index % 2
    rank = (1 - odd) * (index // 2) + odd * (size - (index + 1) // 2)

    def place(r):
        high = r // (size // 2)
        return (1 - high) * 2 * r + high * (2 * (size - r) - 1)

    return place((rank + 1) % size), place((rank + size - 1) % size)


def path_kernel(
    plan, single, flags_ref, x_hbm, g_hbm, r_hbm, m_hbm, v_hbm, arr_hbm, own_hbm, *scratch
):
    (xg, params, hidden, first, second, pseudo) = scratch[:6]
    if single:
        (raw, swapped, cross_in, own_in, cross_out, own_out) = scratch[6:12]
    (load_sem, moment_sem, send_sem, recv_sem, side_send, side_recv, out_send, out_recv, keep_sem) = (
        scratch[-9:]
    )
    n, shard, half = plan.ring, plan.shard, plan.half
    features, owned, tile, tiles = plan.features, plan.owned, plan.tile, plan.tiles
    path = lax.axis_index("path")
    place = lax.axis_index("fsdp")
    ahead, behind = ring_neighbours(place, n)
    core = path % 2
    sibling = path + 1 - 2 * core
    lanes = 1 if single else 2

    barrier = pltpu.get_barrier_semaphore()
    for spot in (ahead, behind):
        pl.semaphore_signal(
            barrier, inc=1, device_id={"path": path, "fsdp": spot}, device_id_type=MESH
        )
    for k in range(1, plan.paths):
        pl.semaphore_signal(
            barrier,
            inc=1,
            device_id={"path": (path + k) % plan.paths, "fsdp": place},
            device_id_type=MESH,
        )

    def moments(t, slot):
        cols = pl.ds(pl.multiple_of(t * tile, tile), tile)
        return (
            pltpu.make_async_copy(m_hbm.at[:, cols], first.at[slot], moment_sem.at[0, slot]),
            pltpu.make_async_copy(v_hbm.at[:, cols], second.at[slot], moment_sem.at[1, slot]),
        )

    if single:
        loads = (
            pltpu.make_async_copy(x_hbm, raw.at[0], load_sem.at[0]),
            pltpu.make_async_copy(g_hbm, raw.at[1], load_sem.at[1]),
        )
    else:
        loads = (
            pltpu.make_async_copy(x_hbm, xg.at[0, pl.ds(0, shard)], load_sem.at[0]),
            pltpu.make_async_copy(g_hbm, xg.at[1, pl.ds(0, shard)], load_sem.at[1]),
        )
    for load in loads:
        load.start()
    load_params = pltpu.make_async_copy(r_hbm, params, load_sem.at[2])
    load_params.start()
    for load in moments(0, 0):
        load.start()
    pl.semaphore_wait(barrier, plan.paths + 1)
    for load in loads:
        load.wait()

    def ring_copy(step, lane, way):
        array = core if single else lane
        source = pl.ds(pl.multiple_of((step - 1) * shard + way * half, half), half)
        target = pl.ds(pl.multiple_of(step * shard + way * half, half), half)
        return pltpu.make_async_remote_copy(
            src_ref=xg.at[array, source],
            dst_ref=xg.at[array, target],
            send_sem=send_sem.at[lane, way, step],
            recv_sem=recv_sem.at[lane, way, step],
            device_id={"path": path, "fsdp": behind if way else ahead},
            device_id_type=MESH,
        )

    def side_copy(slot, array):
        rows = pl.ds(pl.multiple_of(slot * shard, shard), shard)
        return pltpu.make_async_remote_copy(
            src_ref=xg.at[array, rows],
            dst_ref=xg.at[array, rows],
            send_sem=side_send.at[slot],
            recv_sem=side_recv.at[slot],
            device_id={"path": sibling, "fsdp": place},
            device_id_type=MESH,
        )

    if single:
        active = lead_of(flags_ref, path // 2) == path
        swap = pltpu.make_async_remote_copy(
            src_ref=raw.at[1 - core],
            dst_ref=swapped,
            send_sem=load_sem.at[3],
            recv_sem=load_sem.at[4],
            device_id={"path": sibling, "fsdp": place},
            device_id_type=MESH,
        )
        swap.start()
        swap.wait()
        xg[core, 0:shard] = jnp.where(active, raw[core], swapped[...])

    load_params.wait()

    def forward(j):
        rows = pl.ds(pl.multiple_of(j * plan.batch, plan.batch), plan.batch)

        def unit(u, carry):
            strip = pl.ds(pl.multiple_of(u * plan.units, plan.units), plan.units)
            nt = (((1,), (1,)), ((), ()))
            pre = lax.dot_general(
                params[strip, 0:features], xg[0, rows], nt, preferred_element_type=jnp.float32
            ) * (features**-0.5)
            act, slope = gelu_pair(pre)
            hidden[1, strip, rows] = act.astype(jnp.bfloat16)
            back = lax.dot_general(
                params[strip, features : 2 * features],
                xg[1, rows],
                nt,
                preferred_element_type=jnp.float32,
            ) * ((SETS * UNIT) ** -0.5)
            hidden[0, strip, rows] = (back * slope).astype(jnp.bfloat16)
            return carry

        lax.fori_loop(0, plan.rows // plan.units, unit, 0)

    def gather_batch(j, carry):
        for i in range(plan.group):
            k = j * plan.group + i

            @pl.when(k > 0)
            def _():
                for lane in range(lanes):
                    for way in range(2):
                        ring_copy(k, lane, way).wait_recv()

            @pl.when(k < n - 1)
            def _():
                for lane in range(lanes):
                    for way in range(2):
                        ring_copy(k + 1, lane, way).start()

            if single:
                side_copy(k, core).start()
        if single:
            for i in range(plan.group):
                side_copy(j * plan.group + i, 1 - core).wait_recv()
        forward(j)
        return carry

    lax.fori_loop(0, n // plan.group, gather_batch, 0)

    def cols_of(t):
        return pl.ds(pl.multiple_of(t * tile, tile), tile)

    def rows_of(p):
        return pl.ds(pl.multiple_of(p * owned, owned), owned)

    chip = path // 2
    far = (1 - chip) * 2

    def out_copy(t, k):
        owner = (path + k) % plan.paths
        return pltpu.make_async_remote_copy(
            src_ref=pseudo.at[rows_of(owner), cols_of(t)],
            dst_ref=arr_hbm.at[path, :, cols_of(t)],
            send_sem=out_send.at[t, k],
            recv_sem=out_recv.at[t, k],
            device_id={"path": owner, "fsdp": place},
            device_id_type=MESH,
        )

    def keep_copy(t):
        return pltpu.make_async_copy(
            pseudo.at[rows_of(path), cols_of(t)],
            arr_hbm.at[path, :, cols_of(t)],
            keep_sem.at[0, t],
        )

    def share_copy(t, which):
        owner = (far + 1 - core) if which == 0 else sibling
        return pltpu.make_async_remote_copy(
            src_ref=pseudo.at[rows_of(owner), cols_of(t)],
            dst_ref=(cross_in if which == 0 else own_in).at[t],
            send_sem=out_send.at[t, which],
            recv_sem=out_recv.at[t, which],
            device_id={"path": sibling, "fsdp": place},
            device_id_type=MESH,
        )

    def cross_copy(t):
        return pltpu.make_async_remote_copy(
            src_ref=cross_out.at[t],
            dst_ref=arr_hbm.at[chip, :, cols_of(t)],
            send_sem=out_send.at[t, 2],
            recv_sem=out_recv.at[t, 2],
            device_id={"path": far + core, "fsdp": place},
            device_id_type=MESH,
        )

    def near_copy(t):
        return pltpu.make_async_copy(
            own_out.at[t], arr_hbm.at[chip, :, cols_of(t)], keep_sem.at[0, t]
        )

    def late_copy(t):
        return pltpu.make_async_copy(
            pseudo.at[pl.ds(pl.multiple_of(far * owned, 2 * owned), 2 * owned), cols_of(t)],
            own_hbm.at[:, cols_of(t)],
            keep_sem.at[1, t],
        )

    def pick(t):
        share_copy(t, 0).wait_recv()
        cross_out[t] = jnp.where(active, pseudo[rows_of(far + core), cols_of(t)], cross_in[t])
        cross_copy(t).start()
        share_copy(t, 1).wait_recv()
        own_out[t] = jnp.where(active, pseudo[rows_of(path), cols_of(t)], own_in[t])
        near_copy(t).start()

    def grad_tile(t, carry):
        slot = t % 2

        @pl.when(t + 1 < tiles)
        def _():
            for load in moments(t + 1, 1 - slot):
                load.start()

        for load in moments(t, slot):
            load.wait()
        side = t // (tiles // 2)
        scale = jnp.where(side == 0, features**-0.5, (SETS * UNIT) ** -0.5).astype(jnp.float32)
        token_cols = pl.ds(pl.multiple_of(t % (tiles // 2) * tile, tile), tile)

        def unit(u, inner):
            strip = pl.ds(pl.multiple_of(u * plan.units, plan.units), plan.units)
            grads = (
                jnp.dot(
                    hidden[side, strip, :],
                    xg[side, :, token_cols],
                    preferred_element_type=jnp.float32,
                )
                * scale
            )
            pseudo[strip, cols_of(t)] = adam_delta(
                grads, first[slot, strip, :], second[slot, strip, :], params[strip, cols_of(t)]
            )
            return inner

        lax.fori_loop(0, plan.rows // plan.units, unit, 0)
        if single:
            share_copy(t, 0).start()
            share_copy(t, 1).start()
            late_copy(t).start()

            @pl.when(t > 0)
            def _():
                pick(t - 1)
        else:
            for k in range(plan.paths - 1, 0, -1):
                out_copy(t, k).start()
            keep_copy(t).start()
        return carry

    lax.fori_loop(0, tiles, grad_tile, 0)
    if single:
        pick(tiles - 1)

    def drain_ring(k, carry):
        for lane in range(lanes):
            for way in range(2):
                ring_copy(k, lane, way).wait_send()
        return carry

    lax.fori_loop(1, n, drain_ring, 0)
    if single:

        def drain_side(k, carry):
            side_copy(k, core).wait_send()
            return carry

        lax.fori_loop(0, n, drain_side, 0)

    def drain(t, carry):
        if single:
            share_copy(t, 0).wait_send()
            share_copy(t, 1).wait_send()
            late_copy(t).wait()
            near_copy(t).wait()
            cross_copy(t).wait()
        else:
            for k in range(1, plan.paths):
                out_copy(t, k).wait()
            keep_copy(t).wait()
        return carry

    lax.fori_loop(0, tiles, drain, 0)


def run_path(plan, single, flags, x, g, r, m, v):
    bf16 = jnp.bfloat16
    width, tile, tiles = plan.width, plan.tile, plan.tiles
    scratch = [
        pltpu.VMEM((2, plan.tokens, plan.features), bf16),
        pltpu.VMEM((plan.rows, width), bf16),
        pltpu.VMEM((2, plan.rows, plan.tokens), bf16),
        pltpu.VMEM((2, plan.rows, tile), bf16),
        pltpu.VMEM((2, plan.rows, tile), bf16),
        pltpu.VMEM((plan.rows, width), bf16),
    ]
    if single:
        scratch += [
            pltpu.VMEM((2, plan.shard, plan.features), bf16),
            pltpu.VMEM((plan.shard, plan.features), bf16),
        ] + [pltpu.VMEM((tiles, plan.owned, tile), bf16)] * 4
    lanes = 1 if single else 2
    outs = 3 if single else plan.paths
    dma = pltpu.SemaphoreType.DMA
    scratch += [
        dma((5,)),
        dma((2, 2)),
        dma((lanes, 2, plan.ring)),
        dma((lanes, 2, plan.ring)),
        dma((plan.ring,)),
        dma((plan.ring,)),
        dma((tiles, outs)),
        dma((tiles, outs)),
        dma((2, tiles)),
    ]
    sources = 2 if single else plan.paths
    flops = 8 * plan.tokens * plan.features * plan.rows
    shapes = [jax.ShapeDtypeStruct((sources, plan.owned, width), bf16)]
    if single:
        shapes.append(jax.ShapeDtypeStruct((2 * plan.owned, width), bf16))
    body = functools.partial(path_kernel, plan, single)
    if not single:
        inner = body

        def body(flags_ref, x, g, r, m, v, arr, *rest):
            inner(flags_ref, x, g, r, m, v, arr, None, *rest)

    anywhere = pl.BlockSpec(memory_space=pl.ANY)
    return pl.pallas_call(
        body,
        out_shape=shapes,
        in_specs=[pl.BlockSpec(memory_space=pltpu.SMEM)] + [anywhere] * 5,
        out_specs=[anywhere] * len(shapes),
        scratch_shapes=scratch,
        compiler_params=pltpu.CompilerParams(
            collective_id=0 if single else 1,
            has_side_effects=True,
            vmem_limit_bytes=63 * 1024 * 1024,
        ),
        cost_estimate=pl.CostEstimate(
            flops=flops, bytes_accessed=8 * plan.rows * width, transcendentals=0
        ),
        name="single_path" if single else "both_paths",
    )(flags, x, g, r, m, v)


def refreshed(total, tally, common, inertia):
    average = total / tally
    inertia = INERTIA_FACTOR * inertia + average
    expert = common - GLOBAL_LEARNING * (average + INERTIA_FACTOR * inertia)
    return expert, inertia


def lead_of(flags_ref, chip):
    return 2 * chip + jnp.where(flags_ref[2 * chip + 1] == 1, 1, 0)


def late_of(member_ref, flags_ref, at, owner_chip):
    far = 2 * (1 - owner_chip)
    near = member_ref[lead_of(flags_ref, owner_chip), at]
    shared = member_ref[far, at]
    return jnp.where(shared == member_ref[far + 1, at], shared, near)


def local_call(body, grid, in_specs, out_specs, out_shape, scalars, arrays, aliases=None):
    size = sum(array.size * array.dtype.itemsize for array in arrays)
    return pl.pallas_call(
        body,
        grid_spec=pltpu.PrefetchScalarGridSpec(
            num_scalar_prefetch=len(scalars), grid=grid, in_specs=in_specs, out_specs=out_specs
        ),
        out_shape=out_shape,
        input_output_aliases=aliases or {},
        compiler_params=pltpu.CompilerParams(vmem_limit_bytes=56 * 1024 * 1024),
        cost_estimate=pl.CostEstimate(flops=size, bytes_accessed=size, transcendentals=0),
    )(*scalars, *arrays)


ANYWHERE = pl.BlockSpec(memory_space=pl.ANY)


def pick_early(scalars, common, inertia):
    sets, _, units, width = common.shape
    step = divisor(width, 2048)

    def body(member_ref, flags_ref, spot_ref, common_ref, inertia_ref, out):
        expert, _ = refreshed(0.0, 1.0, common_ref[0, 0], inertia_ref[0, 0])
        out[0] = expert.astype(jnp.bfloat16)

    def at(j, t, member_ref, flags_ref, spot_ref):
        spot = spot_ref[0]
        late = late_of(member_ref, flags_ref, spot * sets + j, spot // 2)
        return (j, 1 - late, 0, t)

    return local_call(
        body,
        (sets, width // step),
        [pl.BlockSpec((1, 1, units, step), at)] * 2,
        pl.BlockSpec((1, units, step), lambda j, t, *_: (j, 0, t)),
        jax.ShapeDtypeStruct((sets, units, width), jnp.bfloat16),
        scalars,
        [common, inertia],
    )


def finish_set(scalars, common, inertia, arrived, j, single, paths, shape, partial):
    sets, choices, units, width = common.shape
    sources = arrived.shape[0]
    step = divisor(width, 1024)
    sends = 2 if single else paths - 1

    def body(member_ref, flags_ref, spot_ref, shares, common_ref, inertia_ref, *refs):
        expert_out, inertia_out, returned, *outs = refs[-3 - sends :]
        spot = spot_ref[0]
        at = spot * sets + j
        updated = []
        for c in range(choices):
            total, count = 0.0, 0.0
            for p in range(paths):
                count += jnp.where((flags_ref[p] == 1) & (member_ref[p, at] == c), 1.0, 0.0)
            for q in range(sources):
                p = lead_of(flags_ref, q) if single else q
                weight = jnp.where((flags_ref[p] == 1) & (member_ref[p, at] == c), 1.0, 0.0)
                total = total + weight * shares[q].astype(jnp.float32)
            expert, moved = refreshed(
                total, jnp.maximum(count, 1.0), common_ref[0, c], inertia_ref[0, c]
            )
            expert_out[0, c] = expert
            inertia_out[0, c] = moved
            updated.append(expert.astype(jnp.bfloat16))

        def choose(index):
            chosen = updated[0]
            for c in range(1, choices):
                chosen = jnp.where(index == c, updated[c], chosen)
            return chosen

        returned[0, 0] = choose(member_ref[spot, at])
        if single:
            outs[0][...] = choose(late_of(member_ref, flags_ref, at, spot // 2))
            outs[1][...] = choose(member_ref[spot ^ 1, at])
        else:
            for k in range(1, paths):
                outs[k - 1][...] = choose(member_ref[spot ^ k, at])

    block = pl.BlockSpec((1, choices, units, step), lambda t, *_: (j, 0, 0, t))
    flat = pl.BlockSpec((units, step), lambda t, *_: (0, t))
    own = pl.BlockSpec((1, 1, units, step), lambda t, m, f, spot: (0, spot[0] * sets + j, 0, t))
    arrays = [arrived, common, inertia] + list(partial)
    return local_call(
        body,
        (width // step,),
        [pl.BlockSpec((sources, units, step), lambda t, *_: (0, j, t)), block, block]
        + [ANYWHERE] * len(partial),
        [block, block, own] + [flat] * sends,
        [jax.ShapeDtypeStruct(common.shape, jnp.float32)] * 2
        + [jax.ShapeDtypeStruct(shape, jnp.bfloat16)]
        + [jax.ShapeDtypeStruct((units, width), jnp.bfloat16)] * sends,
        scalars,
        arrays,
        {6 + i: i for i in range(len(partial))},
    )


def place_block(scalars, returned, block, j, sets, k):
    _, _, units, width = returned.shape
    step = divisor(width, 2048)

    def body(member_ref, flags_ref, spot_ref, block_ref, _, out):
        out[0, 0] = block_ref[...]

    return local_call(
        body,
        (width // step,),
        [pl.BlockSpec((units, step), lambda t, *_: (0, t)), ANYWHERE],
        pl.BlockSpec(
            (1, 1, units, step), lambda t, m, f, spot: (0, (spot[0] ^ k) * sets + j, 0, t)
        ),
        jax.ShapeDtypeStruct(returned.shape, jnp.bfloat16),
        scalars,
        [block, returned],
        {4: 0},
    )


def place_far(scalars, returned, late_block, early_block, mine, j, sets, turn):
    _, _, units, width = returned.shape
    step = divisor(width, 2048)

    def serving(spot):
        return (spot % 2) ^ turn

    def place(spot):
        return (2 * (1 - spot // 2) + serving(spot)) * sets + j

    def body(member_ref, flags_ref, spot_ref, late_ref, early_ref, mine_ref, _, out):
        spot = spot_ref[0]
        at = place(spot)
        gain = jnp.where(flags_ref[spot] == 1, GLOBAL_LEARNING * (1.0 + INERTIA_FACTOR), 0.0)
        late = late_of(member_ref, flags_ref, at, 1 - spot // 2)
        quiet = early_ref[0].astype(jnp.float32) - gain * mine_ref[...].astype(jnp.float32)
        out[0, 0] = jnp.where(
            member_ref[spot, at] == late, late_ref[...], quiet.astype(jnp.bfloat16)
        )

    return local_call(
        body,
        (width // step,),
        [
            pl.BlockSpec((units, step), lambda t, *_: (0, t)),
            pl.BlockSpec((1, units, step), lambda t, *_: (j, 0, t)),
            pl.BlockSpec((units, step), lambda t, m, f, spot: (serving(spot[0]) * sets + j, t)),
            ANYWHERE,
        ],
        pl.BlockSpec((1, 1, units, step), lambda t, m, f, spot: (0, place(spot[0]), 0, t)),
        jax.ShapeDtypeStruct(returned.shape, jnp.bfloat16),
        scalars,
        [late_block, early_block, mine, returned],
        {6: 0},
    )


def per_device(
    input_activation_matrix,
    output_sensitivity,
    trajectory_initial_parameters,
    trajectory_gradient_average,
    trajectory_squared_average,
    common_expert_parameters,
    outer_inertia,
    trajectory_membership,
    punctual_flags,
):
    set_count, local_units, row_width = trajectory_initial_parameters.shape[1:]
    rows = set_count * local_units
    path_count = lax.axis_size("path")
    owned_sets = set_count // path_count
    choices = common_expert_parameters.shape[1]
    plan = Plan(
        path_count,
        lax.axis_size("fsdp"),
        input_activation_matrix.shape[1],
        row_width // 2,
        rows,
    )
    x, g = input_activation_matrix[0], output_sensitivity[0]
    r, m, v = (
        array[0].reshape(rows, row_width)
        for array in (
            trajectory_initial_parameters,
            trajectory_gradient_average,
            trajectory_squared_average,
        )
    )
    common, inertia = common_expert_parameters, outer_inertia
    flags = punctual_flags
    scalars = (
        trajectory_membership,
        flags,
        lax.axis_index("path").astype(jnp.int32)[None],
    )
    shape = (1, set_count, local_units, row_width)

    def finish(arrived, alone, j, partial):
        return finish_set(
            scalars, common, inertia, arrived, j, alone, path_count, shape, partial
        )

    def both():
        (arrived,) = run_path(plan, False, flags, x, g, r, m, v)
        hops = list(range(path_count - 1, 0, -1))
        trade = {k: [(p, p ^ k) for p in range(path_count)] for k in hops}
        moved, partial = [], ()
        for j in range(owned_sets):
            *partial, = finish(arrived, False, j, partial)
            blocks, partial = partial[3:], partial[:3]
            moved.append({k: lax.ppermute(blocks[k - 1], "path", trade[k]) for k in hops})
        experts, inertias, returned = partial
        for j in range(owned_sets):
            for k in reversed(hops):
                returned = place_block(scalars, returned, moved[j][k], j, owned_sets, k)
        return experts, inertias, returned

    def single():
        cross = [(p, p ^ 2) for p in range(path_count)]
        swap = [(p, p ^ 1) for p in range(path_count)]
        base = pick_early(scalars, common, inertia)
        early = lax.ppermute(base, "path", cross)
        arrived, mine = run_path(plan, True, flags, x, g, r, m, v)
        still = (early, lax.ppermute(early, "path", swap))
        moved, beside, partial = [], [], ()
        for j in range(owned_sets):
            *partial, late_block, near_block = finish(arrived, True, j, partial)
            sent = lax.ppermute(late_block, "path", cross)
            moved.append((sent, lax.ppermute(sent, "path", swap)))
            beside.append(lax.ppermute(near_block, "path", swap))
        experts, inertias, returned = partial
        for j in range(owned_sets):
            returned = place_block(scalars, returned, beside[j], j, owned_sets, 1)
        for j in range(owned_sets):
            for turn in range(2):
                returned = place_far(
                    scalars, returned, moved[j][turn], still[turn], mine, j, owned_sets, turn
                )
        return experts, inertias, returned

    if path_count == 4 and choices == 2:
        lone = jnp.max(flags.reshape(2, 2).sum(axis=1)) <= 1
        return lax.cond(lone, single, both)
    return both()


def solution(mesh):
    placed = (
        P("path", "fsdp", None),
        P("path", "fsdp", None),
        P("path", None, "fsdp", None),
        P("path", None, "fsdp", None),
        P("path", None, "fsdp", None),
        P("path", None, "fsdp", None),
        P("path", None, "fsdp", None),
        P(),
        P(),
    )
    return jax.shard_map(
        per_device,
        mesh=mesh,
        in_specs=placed,
        out_specs=(
            P("path", None, "fsdp", None),
            P("path", None, "fsdp", None),
            P("path", None, "fsdp", None),
        ),
        check_vma=False,
    )
```

```python
import functools

import jax
import jax.numpy as jnp
from jax import lax
from jax.experimental import pallas as pl
from jax.experimental.pallas import tpu as pltpu
from jax.sharding import PartitionSpec as P


UNIT = 1024
SETS = 8
STEP = 1000


BETA_ONE = 0.9
BETA_TWO = 0.999
ADAM_EPS = 1e-08
INNER_RATE = 0.05
DECAY = 0.1
GLOBAL_LEARNING = 0.7
INERTIA_FACTOR = 0.9

MESH = pl.DeviceIdType.MESH
GELU_ROOT = 0.7978845608028654
GELU_CUBE = 0.044715


def adam_delta(grads, first, second, start):
    corr_one = 1.0 - BETA_ONE**STEP
    corr_two = 1.0 - BETA_TWO**STEP
    first_new = BETA_ONE * first.astype(jnp.float32) + (1.0 - BETA_ONE) * grads
    second_new = BETA_TWO * second.astype(jnp.float32) + (1.0 - BETA_TWO) * grads * grads
    direction = first_new / corr_one / (jnp.sqrt(second_new / corr_two) + ADAM_EPS)
    return (INNER_RATE * (direction + DECAY * start.astype(jnp.float32))).astype(jnp.bfloat16)


def adam_folded(product, scale, first, second, start):
    corr_one = 1.0 - BETA_ONE**STEP
    corr_two = 1.0 - BETA_TWO**STEP
    up = (BETA_ONE / corr_one) * first.astype(jnp.float32) + (
        (1.0 - BETA_ONE) / corr_one * scale
    ) * product
    spread = (BETA_TWO / corr_two) * second.astype(jnp.float32) + (
        (1.0 - BETA_TWO) / corr_two * scale * scale
    ) * (product * product)
    down = spread * lax.rsqrt(spread) + ADAM_EPS
    return (
        INNER_RATE * (up / down) + (INNER_RATE * DECAY) * start.astype(jnp.float32)
    ).astype(jnp.bfloat16)


def gelu_pair(pre):
    square = pre * pre
    tanh = jnp.tanh(GELU_ROOT * pre * (1.0 + GELU_CUBE * square))
    half = 0.5 * (1.0 + tanh)
    slope = half + 0.5 * pre * (1.0 - tanh * tanh) * GELU_ROOT * (1.0 + 3.0 * GELU_CUBE * square)
    return pre * half, slope


def divisor(total, wanted):
    size = min(total, wanted)
    while total % size:
        size //= 2
    return size


class Plan:
    def __init__(self, paths, ring, shard, features, rows):
        self.paths, self.ring, self.shard = paths, ring, shard
        self.features, self.width, self.rows = features, 2 * features, rows
        self.tokens = ring * shard
        self.half = shard // 2
        self.owned = rows // paths
        self.group = 1
        while (self.group * shard) % 128:
            self.group *= 2
        self.batch = self.group * shard
        self.tile = divisor(features, 512)
        self.tiles = self.width // self.tile
        self.units = divisor(rows, 256)
        self.pieces = 2 if self.half % 32 == 0 else 1
        self.slots = 3
        self.chunk = 256 if self.tokens % 256 == 0 else self.tokens


def ring_neighbours(index, size):
    odd = index % 2
    rank = (1 - odd) * (index // 2) + odd * (size - (index + 1) // 2)

    def place(r):
        high = r // (size // 2)
        return (1 - high) * 2 * r + high * (2 * (size - r) - 1)

    return place((rank + 1) % size), place((rank + size - 1) % size)


def path_kernel(
    plan, single, flags_ref, x_hbm, g_hbm, r_hbm, m_hbm, v_hbm, arr_hbm, own_hbm, *scratch
):
    (xg, params, hidden, first, second, pseudo) = scratch[:6]
    if single:
        (raw, swapped, cross_in, own_in, cross_out, own_out) = scratch[6:12]
    (load_sem, moment_sem, send_sem, recv_sem, side_send, side_recv, out_send, out_recv, keep_sem) = (
        scratch[-9:]
    )
    n, shard, half = plan.ring, plan.shard, plan.half
    features, owned, tile, tiles = plan.features, plan.owned, plan.tile, plan.tiles
    path = lax.axis_index("path")
    place = lax.axis_index("fsdp")
    ahead, behind = ring_neighbours(place, n)
    core = path % 2
    sibling = path + 1 - 2 * core
    lanes = 1 if single else 2

    barrier = pltpu.get_barrier_semaphore()
    for spot in (ahead, behind):
        pl.semaphore_signal(
            barrier, inc=1, device_id={"path": path, "fsdp": spot}, device_id_type=MESH
        )
    for k in range(1, plan.paths):
        pl.semaphore_signal(
            barrier,
            inc=1,
            device_id={"path": (path + k) % plan.paths, "fsdp": place},
            device_id_type=MESH,
        )

    def moments(t, slot):
        cols = pl.ds(pl.multiple_of(t * tile, tile), tile)
        return (
            pltpu.make_async_copy(m_hbm.at[:, cols], first.at[slot], moment_sem.at[0, slot]),
            pltpu.make_async_copy(v_hbm.at[:, cols], second.at[slot], moment_sem.at[1, slot]),
        )

    if single:
        loads = (
            pltpu.make_async_copy(x_hbm, raw.at[0], load_sem.at[0]),
            pltpu.make_async_copy(g_hbm, raw.at[1], load_sem.at[1]),
        )
    else:
        loads = (
            pltpu.make_async_copy(x_hbm, xg.at[0, pl.ds(0, shard)], load_sem.at[0]),
            pltpu.make_async_copy(g_hbm, xg.at[1, pl.ds(0, shard)], load_sem.at[1]),
        )
    for load in loads:
        load.start()
    load_params = pltpu.make_async_copy(r_hbm, params, load_sem.at[2])
    load_params.start()
    for load in moments(0, 0):
        load.start()
    pl.semaphore_wait(barrier, plan.paths + 1)
    for load in loads:
        load.wait()

    def ring_copy(step, lane, way):
        array = core if single else lane
        source = pl.ds(pl.multiple_of((step - 1) * shard + way * half, half), half)
        target = pl.ds(pl.multiple_of(step * shard + way * half, half), half)
        return pltpu.make_async_remote_copy(
            src_ref=xg.at[array, source],
            dst_ref=xg.at[array, target],
            send_sem=send_sem.at[lane, way, step],
            recv_sem=recv_sem.at[lane, way, step],
            device_id={"path": path, "fsdp": behind if way else ahead},
            device_id_type=MESH,
        )

    def side_copy(slot, array):
        rows = pl.ds(pl.multiple_of(slot * shard, shard), shard)
        return pltpu.make_async_remote_copy(
            src_ref=xg.at[array, rows],
            dst_ref=xg.at[array, rows],
            send_sem=side_send.at[slot],
            recv_sem=side_recv.at[slot],
            device_id={"path": sibling, "fsdp": place},
            device_id_type=MESH,
        )

    if single:
        active = lead_of(flags_ref, path // 2) == path
        swap = pltpu.make_async_remote_copy(
            src_ref=raw.at[1 - core],
            dst_ref=swapped,
            send_sem=load_sem.at[3],
            recv_sem=load_sem.at[4],
            device_id={"path": sibling, "fsdp": place},
            device_id_type=MESH,
        )
        swap.start()
        swap.wait()
        xg[core, 0:shard] = jnp.where(active, raw[core], swapped[...])

    load_params.wait()

    def forward(j):
        rows = pl.ds(pl.multiple_of(j * plan.batch, plan.batch), plan.batch)

        def unit(u, carry):
            strip = pl.ds(pl.multiple_of(u * plan.units, plan.units), plan.units)
            nt = (((1,), (1,)), ((), ()))
            pre = lax.dot_general(
                params[strip, 0:features], xg[0, rows], nt, preferred_element_type=jnp.float32
            ) * (features**-0.5)
            act, slope = gelu_pair(pre)
            hidden[1, strip, rows] = act.astype(jnp.bfloat16)
            back = lax.dot_general(
                params[strip, features : 2 * features],
                xg[1, rows],
                nt,
                preferred_element_type=jnp.float32,
            ) * ((SETS * UNIT) ** -0.5)
            hidden[0, strip, rows] = (back * slope).astype(jnp.bfloat16)
            return carry

        lax.fori_loop(0, plan.rows // plan.units, unit, 0)

    def gather_batch(j, carry):
        for i in range(plan.group):
            k = j * plan.group + i

            @pl.when(k > 0)
            def _():
                for lane in range(lanes):
                    for way in range(2):
                        ring_copy(k, lane, way).wait_recv()

            @pl.when(k < n - 1)
            def _():
                for lane in range(lanes):
                    for way in range(2):
                        ring_copy(k + 1, lane, way).start()

            if single:
                side_copy(k, core).start()
        if single:
            for i in range(plan.group):
                side_copy(j * plan.group + i, 1 - core).wait_recv()
        forward(j)
        return carry

    lax.fori_loop(0, n // plan.group, gather_batch, 0)

    def cols_of(t):
        return pl.ds(pl.multiple_of(t * tile, tile), tile)

    def rows_of(p):
        return pl.ds(pl.multiple_of(p * owned, owned), owned)

    chip = path // 2
    far = (1 - chip) * 2

    def out_copy(t, k):
        owner = (path + k) % plan.paths
        return pltpu.make_async_remote_copy(
            src_ref=pseudo.at[rows_of(owner), cols_of(t)],
            dst_ref=arr_hbm.at[path, :, cols_of(t)],
            send_sem=out_send.at[t, k],
            recv_sem=out_recv.at[t, k],
            device_id={"path": owner, "fsdp": place},
            device_id_type=MESH,
        )

    def keep_copy(t):
        return pltpu.make_async_copy(
            pseudo.at[rows_of(path), cols_of(t)],
            arr_hbm.at[path, :, cols_of(t)],
            keep_sem.at[0, t],
        )

    def share_copy(t, which):
        owner = (far + 1 - core) if which == 0 else sibling
        return pltpu.make_async_remote_copy(
            src_ref=pseudo.at[rows_of(owner), cols_of(t)],
            dst_ref=(cross_in if which == 0 else own_in).at[t],
            send_sem=out_send.at[t, which],
            recv_sem=out_recv.at[t, which],
            device_id={"path": sibling, "fsdp": place},
            device_id_type=MESH,
        )

    def cross_copy(t):
        return pltpu.make_async_remote_copy(
            src_ref=cross_out.at[t],
            dst_ref=arr_hbm.at[chip, :, cols_of(t)],
            send_sem=out_send.at[t, 2],
            recv_sem=out_recv.at[t, 2],
            device_id={"path": far + core, "fsdp": place},
            device_id_type=MESH,
        )

    def near_copy(t):
        return pltpu.make_async_copy(
            own_out.at[t], arr_hbm.at[chip, :, cols_of(t)], keep_sem.at[0, t]
        )

    def late_copy(t):
        return pltpu.make_async_copy(
            pseudo.at[pl.ds(pl.multiple_of(far * owned, 2 * owned), 2 * owned), cols_of(t)],
            own_hbm.at[:, cols_of(t)],
            keep_sem.at[1, t],
        )

    def pick(t):
        share_copy(t, 0).wait_recv()
        cross_out[t] = jnp.where(active, pseudo[rows_of(far + core), cols_of(t)], cross_in[t])
        cross_copy(t).start()
        share_copy(t, 1).wait_recv()
        own_out[t] = jnp.where(active, pseudo[rows_of(path), cols_of(t)], own_in[t])
        near_copy(t).start()

    def grad_tile(t, carry):
        slot = t % 2

        @pl.when(t + 1 < tiles)
        def _():
            for load in moments(t + 1, 1 - slot):
                load.start()

        for load in moments(t, slot):
            load.wait()
        side = t // (tiles // 2)
        scale = jnp.where(side == 0, features**-0.5, (SETS * UNIT) ** -0.5).astype(jnp.float32)
        token_cols = pl.ds(pl.multiple_of(t % (tiles // 2) * tile, tile), tile)

        def unit(u, inner):
            strip = pl.ds(pl.multiple_of(u * plan.units, plan.units), plan.units)
            grads = (
                jnp.dot(
                    hidden[side, strip, :],
                    xg[side, :, token_cols],
                    preferred_element_type=jnp.float32,
                )
                * scale
            )
            pseudo[strip, cols_of(t)] = adam_delta(
                grads, first[slot, strip, :], second[slot, strip, :], params[strip, cols_of(t)]
            )
            return inner

        lax.fori_loop(0, plan.rows // plan.units, unit, 0)
        if single:
            share_copy(t, 0).start()
            share_copy(t, 1).start()
            late_copy(t).start()

            @pl.when(t > 0)
            def _():
                pick(t - 1)
        else:
            for k in range(plan.paths - 1, 0, -1):
                out_copy(t, k).start()
            keep_copy(t).start()
        return carry

    lax.fori_loop(0, tiles, grad_tile, 0)
    if single:
        pick(tiles - 1)

    def drain_ring(k, carry):
        for lane in range(lanes):
            for way in range(2):
                ring_copy(k, lane, way).wait_send()
        return carry

    lax.fori_loop(1, n, drain_ring, 0)
    if single:

        def drain_side(k, carry):
            side_copy(k, core).wait_send()
            return carry

        lax.fori_loop(0, n, drain_side, 0)

    def drain(t, carry):
        if single:
            share_copy(t, 0).wait_send()
            share_copy(t, 1).wait_send()
            late_copy(t).wait()
            near_copy(t).wait()
            cross_copy(t).wait()
        else:
            for k in range(1, plan.paths):
                out_copy(t, k).wait()
            keep_copy(t).wait()
        return carry

    lax.fori_loop(0, tiles, drain, 0)


def run_path(plan, single, flags, x, g, r, m, v):
    bf16 = jnp.bfloat16
    width, tile, tiles = plan.width, plan.tile, plan.tiles
    scratch = [
        pltpu.VMEM((2, plan.tokens, plan.features), bf16),
        pltpu.VMEM((plan.rows, width), bf16),
        pltpu.VMEM((2, plan.rows, plan.tokens), bf16),
        pltpu.VMEM((2, plan.rows, tile), bf16),
        pltpu.VMEM((2, plan.rows, tile), bf16),
        pltpu.VMEM((plan.rows, width), bf16),
    ]
    if single:
        scratch += [
            pltpu.VMEM((2, plan.shard, plan.features), bf16),
            pltpu.VMEM((plan.shard, plan.features), bf16),
        ] + [pltpu.VMEM((tiles, plan.owned, tile), bf16)] * 4
    lanes = 1 if single else 2
    outs = 3 if single else plan.paths
    dma = pltpu.SemaphoreType.DMA
    scratch += [
        dma((5,)),
        dma((2, 2)),
        dma((lanes, 2, plan.ring)),
        dma((lanes, 2, plan.ring)),
        dma((plan.ring,)),
        dma((plan.ring,)),
        dma((tiles, outs)),
        dma((tiles, outs)),
        dma((2, tiles)),
    ]
    sources = 2 if single else plan.paths
    flops = 8 * plan.tokens * plan.features * plan.rows
    shapes = [jax.ShapeDtypeStruct((sources, plan.owned, width), bf16)]
    if single:
        shapes.append(jax.ShapeDtypeStruct((2 * plan.owned, width), bf16))
    body = functools.partial(path_kernel, plan, single)
    if not single:
        inner = body

        def body(flags_ref, x, g, r, m, v, arr, *rest):
            inner(flags_ref, x, g, r, m, v, arr, None, *rest)

    anywhere = pl.BlockSpec(memory_space=pl.ANY)
    return pl.pallas_call(
        body,
        out_shape=shapes,
        in_specs=[pl.BlockSpec(memory_space=pltpu.SMEM)] + [anywhere] * 5,
        out_specs=[anywhere] * len(shapes),
        scratch_shapes=scratch,
        compiler_params=pltpu.CompilerParams(
            collective_id=0 if single else 1,
            has_side_effects=True,
            vmem_limit_bytes=63 * 1024 * 1024,
        ),
        cost_estimate=pl.CostEstimate(
            flops=flops, bytes_accessed=8 * plan.rows * width, transcendentals=0
        ),
        name="single_path" if single else "both_paths",
    )(flags, x, g, r, m, v)


def survivor_kernel(
    plan, rounds, flags_ref, x_hbm, g_hbm, r_hbm, m_hbm, v_hbm, arr_hbm, own_hbm, *scratch
):
    (xg, params, hidden, first, second, pseudo, raw, swapped) = scratch[:8]
    (cross_in, own_in, cross_out, own_out) = scratch[8:12]
    (load_sem, moment_sem, send_sem, recv_sem, side_send, side_recv, out_send, out_recv, keep_sem) = (
        scratch[12:]
    )
    n, shard, half = plan.ring, plan.shard, plan.half
    features, owned, tile, tiles = plan.features, plan.owned, plan.tile, plan.tiles
    pieces, slots = plan.pieces, plan.slots
    path = lax.axis_index("path")
    place = lax.axis_index("fsdp")
    ahead, behind = ring_neighbours(place, n)
    core, chip = path % 2, path // 2
    sibling = path + 1 - 2 * core
    far = (1 - chip) * 2
    leading = jnp.where(lead_of(flags_ref, chip) == path, 1, 0)

    barrier = pltpu.get_barrier_semaphore()
    partners = [(path, ahead), (path, behind), (sibling, place), (far + core, place)]
    for to_path, to_place in partners:
        pl.semaphore_signal(
            barrier, inc=1, device_id={"path": to_path, "fsdp": to_place}, device_id_type=MESH
        )

    def cols_of(t):
        return pl.ds(pl.multiple_of(t * tile, tile), tile)

    def rows_of(p):
        return pl.ds(pl.multiple_of(p * owned, owned), owned)

    def moments(index):
        cols, slot = cols_of(index % tiles), index % 2
        return (
            pltpu.make_async_copy(m_hbm.at[:, cols], first.at[slot], moment_sem.at[0, slot]),
            pltpu.make_async_copy(v_hbm.at[:, cols], second.at[slot], moment_sem.at[1, slot]),
        )

    loads = (
        pltpu.make_async_copy(x_hbm, raw.at[0], load_sem.at[0]),
        pltpu.make_async_copy(g_hbm, raw.at[1], load_sem.at[1]),
    )
    for load in loads:
        load.start()
    load_params = pltpu.make_async_copy(r_hbm, params, load_sem.at[2])
    load_params.start()
    for load in moments(0):
        load.start()
    pl.semaphore_wait(barrier, len(partners))
    for load in loads:
        load.wait()
    swap = pltpu.make_async_remote_copy(
        src_ref=raw.at[1 - core],
        dst_ref=swapped,
        send_sem=load_sem.at[3],
        recv_sem=load_sem.at[4],
        device_id={"path": sibling, "fsdp": place},
        device_id_type=MESH,
    )
    swap.start()
    swap.wait()
    for turn in range(rounds):
        mine = leading == 1 - turn
        xg[turn, core, 0:shard] = jnp.where(mine, raw[core], swapped[...])

    def ring_copies(turn, step):
        copies = []
        for piece in range(pieces):
            for way in range(2):
                size = half // pieces
                at = way * half + piece * size
                source = pl.ds(pl.multiple_of((step - 1) * shard + at, 16), size)
                target = pl.ds(pl.multiple_of(step * shard + at, 16), size)
                copies.append(
                    pltpu.make_async_remote_copy(
                        src_ref=xg.at[turn, core, source],
                        dst_ref=xg.at[turn, core, target],
                        send_sem=send_sem.at[turn, way * pieces + piece, step],
                        recv_sem=recv_sem.at[turn, way * pieces + piece, step],
                        device_id={"path": path, "fsdp": behind if way else ahead},
                        device_id_type=MESH,
                    )
                )
        return copies

    def side_copy(turn, slot, array):
        rows = pl.ds(pl.multiple_of(slot * shard, shard), shard)
        return pltpu.make_async_remote_copy(
            src_ref=xg.at[turn, array, rows],
            dst_ref=xg.at[turn, array, rows],
            send_sem=side_send.at[turn, slot],
            recv_sem=side_recv.at[turn, slot],
            device_id={"path": sibling, "fsdp": place},
            device_id_type=MESH,
        )

    def begin(turn):
        for copy in ring_copies(turn, 1):
            copy.start()
        side_copy(turn, 0, core).start()

    begin(0)
    load_params.wait()

    def forward(turn, j):
        rows = pl.ds(pl.multiple_of(j * plan.chunk, plan.chunk), plan.chunk)

        def unit(u, carry):
            strip = pl.ds(pl.multiple_of(u * plan.units, plan.units), plan.units)
            nt = (((1,), (1,)), ((), ()))
            pre = lax.dot_general(
                params[strip, 0:features], xg[turn, 0, rows], nt, preferred_element_type=jnp.float32
            ) * (features**-0.5)
            act, slope = gelu_pair(pre)
            hidden[1, strip, rows] = act.astype(jnp.bfloat16)
            back = lax.dot_general(
                params[strip, features : 2 * features],
                xg[turn, 1, rows],
                nt,
                preferred_element_type=jnp.float32,
            ) * ((SETS * UNIT) ** -0.5)
            hidden[0, strip, rows] = (back * slope).astype(jnp.bfloat16)
            return carry

        lax.fori_loop(0, plan.rows // plan.units, unit, 0)

    def share_copy(index, which):
        owner = (far + 1 - core) if which == 0 else sibling
        return pltpu.make_async_remote_copy(
            src_ref=pseudo.at[index % slots, rows_of(owner)],
            dst_ref=(cross_in if which == 0 else own_in).at[index],
            send_sem=out_send.at[index, which],
            recv_sem=out_recv.at[index, which],
            device_id={"path": sibling, "fsdp": place},
            device_id_type=MESH,
        )

    def cross_copy(index):
        return pltpu.make_async_remote_copy(
            src_ref=cross_out.at[index % tiles],
            dst_ref=arr_hbm.at[index // tiles * 2 + chip, :, cols_of(index % tiles)],
            send_sem=out_send.at[index, 2],
            recv_sem=out_recv.at[index, 2],
            device_id={"path": far + core, "fsdp": place},
            device_id_type=MESH,
        )

    def near_copy(index):
        return pltpu.make_async_copy(
            own_out.at[index % tiles],
            arr_hbm.at[index // tiles * 2 + chip, :, cols_of(index % tiles)],
            keep_sem.at[0, index],
        )

    def own_copy(index):
        rows = pl.ds(pl.multiple_of(far * owned, 2 * owned), 2 * owned)
        out = pl.ds(pl.multiple_of(index // tiles * 2 * owned, 2 * owned), 2 * owned)
        return pltpu.make_async_copy(
            pseudo.at[index % slots, rows],
            own_hbm.at[out, cols_of(index % tiles)],
            keep_sem.at[1, index],
        )

    def pick(index):
        mine = leading == 1 - index // tiles

        @pl.when(index >= tiles)
        def _():
            cross_copy(index - tiles).wait_send()
            near_copy(index - tiles).wait()

        slot, t = index % slots, index % tiles
        share_copy(index, 0).wait_recv()
        cross_out[t] = jnp.where(mine, pseudo[slot, rows_of(far + core)], cross_in[index])
        cross_copy(index).start()
        share_copy(index, 1).wait_recv()
        own_out[t] = jnp.where(mine, pseudo[slot, rows_of(path)], own_in[index])
        near_copy(index).start()

    def release(index):
        share_copy(index, 0).wait_send()
        share_copy(index, 1).wait_send()
        own_copy(index).wait()

    def grad_tile(index, carry):
        moment, slot = index % 2, index % slots
        turn, t = index // tiles, index % tiles

        @pl.when(index + 1 < rounds * tiles)
        def _():
            for load in moments(index + 1):
                load.start()

        @pl.when(index >= slots)
        def _():
            release(index - slots)

        for load in moments(index):
            load.wait()
        side = t // (tiles // 2)
        scale = jnp.where(side == 0, features**-0.5, (SETS * UNIT) ** -0.5).astype(jnp.float32)
        token_cols = pl.ds(pl.multiple_of(t % (tiles // 2) * tile, tile), tile)

        def unit(u, inner):
            strip = pl.ds(pl.multiple_of(u * plan.units, plan.units), plan.units)
            product = jnp.dot(
                hidden[side, strip, :],
                xg[turn, side, :, token_cols],
                preferred_element_type=jnp.float32,
            )
            pseudo[slot, strip, :] = adam_folded(
                product,
                scale,
                first[moment, strip, :],
                second[moment, strip, :],
                params[strip, cols_of(t)],
            )
            return inner

        lax.fori_loop(0, plan.rows // plan.units, unit, 0)
        share_copy(index, 0).start()
        share_copy(index, 1).start()
        own_copy(index).start()

        @pl.when(index > 0)
        def _():
            pick(index - 1)

        return carry

    spread = -(-tiles // 4)
    last = rounds * n

    def stage(i, carry):
        turn, k = i // n, i % n

        @pl.when((k > 0) & (i < last))
        def _():
            arrivals = ring_copies(turn, k)

            @pl.when(k < n - 1)
            def _():
                for here, onward in zip(arrivals, ring_copies(turn, k + 1)):
                    here.wait_recv()
                    onward.start()

            @pl.when(k == n - 1)
            def _():
                for here in arrivals:
                    here.wait_recv()

            side_copy(turn, k, core).start()

        if rounds > 1:

            @pl.when((k == n - 1) & (turn + 1 < rounds))
            def _():
                begin(turn + 1)

        @pl.when(i < last)
        def _():
            side_copy(turn, k, 1 - core).wait_recv()

        begun, ended = k * shard // plan.chunk, (k + 1) * shard // plan.chunk
        if rounds == 1:
            low = jnp.where(i == last, 0, tiles)
            high = tiles
        else:
            held = (turn == 1) & (k < 4)
            low = jnp.where(held, k * spread, jnp.where(i == last, tiles, 0))
            high = jnp.where(
                held, jnp.minimum(k * spread + spread, tiles), jnp.where(i == last, 2 * tiles, 0)
            )
            begun = jnp.where((turn == 1) & (k < 6), jnp.where(k == 5, 2, 0), begun)
            ended = jnp.where((turn == 1) & (k < 5), jnp.where(k == 4, 2, 0), ended)
        lax.fori_loop(low, high, grad_tile, 0)

        def ready(j, inner):
            forward(turn, j)
            return inner

        lax.fori_loop(jnp.where(i < last, begun, ended), ended, ready, 0)
        return carry

    lax.fori_loop(0, last + 1, stage, 0)
    pick(rounds * tiles - 1)

    def drain_ring(i, carry):
        turn, k = i // n, i % n
        side_copy(turn, k, core).wait_send()

        @pl.when(k > 0)
        def _():
            for copy in ring_copies(turn, k):
                copy.wait_send()

        return carry

    lax.fori_loop(0, rounds * n, drain_ring, 0)

    def drain(index, carry):
        @pl.when(index >= rounds * tiles - slots)
        def _():
            release(index)

        @pl.when(index >= (rounds - 1) * tiles)
        def _():
            near_copy(index).wait()
            cross_copy(index).wait_send()

        cross_copy(index).wait_recv()
        return carry

    lax.fori_loop(0, rounds * tiles, drain, 0)


def run_survivors(plan, rounds, flags, x, g, r, m, v):
    bf16, dma = jnp.bfloat16, pltpu.SemaphoreType.DMA
    width, tile, tiles = plan.width, plan.tile, plan.tiles
    served = pltpu.VMEM((rounds * tiles, plan.owned, tile), bf16)
    sent = pltpu.VMEM((tiles, plan.owned, tile), bf16)
    scratch = [
        pltpu.VMEM((rounds, 2, plan.tokens, plan.features), bf16),
        pltpu.VMEM((plan.rows, width), bf16),
        pltpu.VMEM((2, plan.rows, plan.tokens), bf16),
        pltpu.VMEM((2, plan.rows, tile), bf16),
        pltpu.VMEM((2, plan.rows, tile), bf16),
        pltpu.VMEM((plan.slots, plan.rows, tile), bf16),
        pltpu.VMEM((2, plan.shard, plan.features), bf16),
        pltpu.VMEM((plan.shard, plan.features), bf16),
        served,
        served,
        sent,
        sent,
        dma((5,)),
        dma((2, 2)),
        dma((rounds, 2 * plan.pieces, plan.ring)),
        dma((rounds, 2 * plan.pieces, plan.ring)),
        dma((rounds, plan.ring)),
        dma((rounds, plan.ring)),
        dma((rounds * tiles, 3)),
        dma((rounds * tiles, 3)),
        dma((2, rounds * tiles)),
    ]
    anywhere = pl.BlockSpec(memory_space=pl.ANY)
    return pl.pallas_call(
        functools.partial(survivor_kernel, plan, rounds),
        out_shape=[
            jax.ShapeDtypeStruct((2 * rounds, plan.owned, width), bf16),
            jax.ShapeDtypeStruct((2 * rounds * plan.owned, width), bf16),
        ],
        in_specs=[pl.BlockSpec(memory_space=pltpu.SMEM)] + [anywhere] * 5,
        out_specs=[anywhere] * 2,
        scratch_shapes=scratch,
        compiler_params=pltpu.CompilerParams(
            collective_id=rounds, has_side_effects=True, vmem_limit_bytes=67043328
        ),
        cost_estimate=pl.CostEstimate(
            flops=8 * plan.tokens * plan.features * plan.rows * rounds,
            bytes_accessed=8 * plan.rows * width,
            transcendentals=0,
        ),
        name="survivors",
    )(flags, x, g, r, m, v)


def refreshed(total, tally, common, inertia):
    average = total / tally
    inertia = INERTIA_FACTOR * inertia + average
    expert = common - GLOBAL_LEARNING * (average + INERTIA_FACTOR * inertia)
    return expert, inertia


def lead_of(flags_ref, chip):
    return 2 * chip + jnp.where(flags_ref[2 * chip + 1] == 1, 1, 0)


def late_of(member_ref, flags_ref, at, owner_chip):
    far = 2 * (1 - owner_chip)
    near = member_ref[lead_of(flags_ref, owner_chip), at]
    shared = member_ref[far, at]
    return jnp.where(shared == member_ref[far + 1, at], shared, near)


def local_call(body, grid, in_specs, out_specs, out_shape, scalars, arrays, aliases=None):
    size = sum(array.size * array.dtype.itemsize for array in arrays)
    return pl.pallas_call(
        body,
        grid_spec=pltpu.PrefetchScalarGridSpec(
            num_scalar_prefetch=len(scalars), grid=grid, in_specs=in_specs, out_specs=out_specs
        ),
        out_shape=out_shape,
        input_output_aliases=aliases or {},
        compiler_params=pltpu.CompilerParams(vmem_limit_bytes=56 * 1024 * 1024),
        cost_estimate=pl.CostEstimate(flops=size, bytes_accessed=size, transcendentals=0),
    )(*scalars, *arrays)


ANYWHERE = pl.BlockSpec(memory_space=pl.ANY)


def pick_early(scalars, common, inertia):
    sets, _, units, width = common.shape
    step = divisor(width, 2048)

    def body(member_ref, flags_ref, spot_ref, common_ref, inertia_ref, out):
        expert, _ = refreshed(0.0, 1.0, common_ref[0, 0], inertia_ref[0, 0])
        out[0] = expert.astype(jnp.bfloat16)

    def at(j, t, member_ref, flags_ref, spot_ref):
        spot = spot_ref[0]
        late = late_of(member_ref, flags_ref, spot * sets + j, spot // 2)
        return (j, 1 - late, 0, t)

    return local_call(
        body,
        (sets, width // step),
        [pl.BlockSpec((1, 1, units, step), at)] * 2,
        pl.BlockSpec((1, units, step), lambda j, t, *_: (j, 0, t)),
        jax.ShapeDtypeStruct((sets, units, width), jnp.bfloat16),
        scalars,
        [common, inertia],
    )


def finish_set(scalars, common, inertia, arrived, j, rounds, paths, shape, partial):
    sets, choices, units, width = common.shape
    sources = arrived.shape[0]
    step = divisor(width, 2048)
    sends = 1 + rounds if rounds else paths - 1

    def body(member_ref, flags_ref, spot_ref, shares, common_ref, inertia_ref, *refs):
        expert_out, inertia_out, returned, *outs = refs[-3 - sends :]
        spot = spot_ref[0]
        at = spot * sets + j
        updated = []
        for c in range(choices):
            total, count = 0.0, 0.0
            for p in range(paths):
                count += jnp.where((flags_ref[p] == 1) & (member_ref[p, at] == c), 1.0, 0.0)
            for q in range(sources):
                p = q
                if rounds:
                    lead = lead_of(flags_ref, q % 2)
                    p = lead if q < 2 else 4 * (q % 2) + 1 - lead
                weight = jnp.where((flags_ref[p] == 1) & (member_ref[p, at] == c), 1.0, 0.0)
                total = total + weight * shares[q].astype(jnp.float32)
            expert, moved = refreshed(
                total, jnp.maximum(count, 1.0), common_ref[0, c], inertia_ref[0, c]
            )
            expert_out[0, c] = expert
            inertia_out[0, c] = moved
            updated.append(expert.astype(jnp.bfloat16))

        def choose(index):
            chosen = updated[0]
            for c in range(1, choices):
                chosen = jnp.where(index == c, updated[c], chosen)
            return chosen

        returned[0, 0] = choose(member_ref[spot, at])
        if rounds:
            late = late_of(member_ref, flags_ref, at, spot // 2)
            outs[0][...] = choose(late)
            outs[1][...] = choose(member_ref[spot ^ 1, at])
            if rounds > 1:
                outs[2][...] = choose(1 - late)
        else:
            for k in range(1, paths):
                outs[k - 1][...] = choose(member_ref[spot ^ k, at])

    block = pl.BlockSpec((1, choices, units, step), lambda t, *_: (j, 0, 0, t))
    flat = pl.BlockSpec((units, step), lambda t, *_: (0, t))
    own = pl.BlockSpec((1, 1, units, step), lambda t, m, f, spot: (0, spot[0] * sets + j, 0, t))
    arrays = [arrived, common, inertia] + list(partial)
    return local_call(
        body,
        (width // step,),
        [pl.BlockSpec((sources, units, step), lambda t, *_: (0, j, t)), block, block]
        + [ANYWHERE] * len(partial),
        [block, block, own] + [flat] * sends,
        [jax.ShapeDtypeStruct(common.shape, jnp.float32)] * 2
        + [jax.ShapeDtypeStruct(shape, jnp.bfloat16)]
        + [jax.ShapeDtypeStruct((units, width), jnp.bfloat16)] * sends,
        scalars,
        arrays,
        {6 + i: i for i in range(len(partial))},
    )


def place_block(scalars, returned, block, j, sets, k):
    _, _, units, width = returned.shape
    step = divisor(width, 2048)

    def body(member_ref, flags_ref, spot_ref, block_ref, _, out):
        out[0, 0] = block_ref[...]

    return local_call(
        body,
        (width // step,),
        [pl.BlockSpec((units, step), lambda t, *_: (0, t)), ANYWHERE],
        pl.BlockSpec(
            (1, 1, units, step), lambda t, m, f, spot: (0, (spot[0] ^ k) * sets + j, 0, t)
        ),
        jax.ShapeDtypeStruct(returned.shape, jnp.bfloat16),
        scalars,
        [block, returned],
        {4: 0},
    )


def needs_other(member, flags, at, owner_chip):
    near, far = 2 * owner_chip, 2 * (1 - owner_chip)
    changed = (flags[near] == 1) & (flags[near + 1] == 1)
    changed &= member[near, at] != member[near + 1, at]
    return changed & (member[far, at] != member[far + 1, at])


def place_far(scalars, returned, late_block, early_block, mine, other_block, j, sets, turn):
    _, _, units, width = returned.shape
    step = divisor(width, 2048)

    def serving(spot):
        return (spot % 2) ^ turn

    def place(spot):
        return (2 * (1 - spot // 2) + serving(spot)) * sets + j

    def body(member_ref, flags_ref, spot_ref, late_ref, early_ref, mine_ref, *refs):
        out = refs[-1]
        spot = spot_ref[0]
        at = place(spot)
        gain = jnp.where(flags_ref[spot] == 1, GLOBAL_LEARNING * (1.0 + INERTIA_FACTOR), 0.0)
        late = late_of(member_ref, flags_ref, at, 1 - spot // 2)
        quiet = early_ref[0].astype(jnp.float32) - gain * mine_ref[...].astype(jnp.float32)
        quiet = quiet.astype(jnp.bfloat16)
        if other_block is not None:
            sent = needs_other(member_ref, flags_ref, at, 1 - spot // 2)
            quiet = jnp.where(sent, refs[0][...], quiet)
        out[0, 0] = jnp.where(member_ref[spot, at] == late, late_ref[...], quiet)

    def mine_at(t, m, flags_ref, spot_ref):
        spot = spot_ref[0]
        behind = jnp.where(lead_of(flags_ref, spot // 2) == spot, 0, 1)
        turn_row = behind * (mine.shape[0] // units - 2 * sets)
        return (turn_row + serving(spot) * sets + j, t)

    flat = pl.BlockSpec((units, step), lambda t, *_: (0, t))
    arrays = [late_block, early_block, mine]
    specs = [
        flat,
        pl.BlockSpec((1, units, step), lambda t, *_: (j, 0, t)),
        pl.BlockSpec((units, step), mine_at),
    ]
    if other_block is not None:
        arrays.append(other_block)
        specs.append(flat)
    return local_call(
        body,
        (width // step,),
        specs + [ANYWHERE],
        pl.BlockSpec((1, 1, units, step), lambda t, m, f, spot: (0, place(spot[0]), 0, t)),
        jax.ShapeDtypeStruct(returned.shape, jnp.bfloat16),
        scalars,
        arrays + [returned],
        {3 + len(arrays): 0},
    )


def per_device(
    input_activation_matrix,
    output_sensitivity,
    trajectory_initial_parameters,
    trajectory_gradient_average,
    trajectory_squared_average,
    common_expert_parameters,
    outer_inertia,
    trajectory_membership,
    punctual_flags,
):
    set_count, local_units, row_width = trajectory_initial_parameters.shape[1:]
    rows = set_count * local_units
    path_count = lax.axis_size("path")
    owned_sets = set_count // path_count
    choices = common_expert_parameters.shape[1]
    plan = Plan(
        path_count,
        lax.axis_size("fsdp"),
        input_activation_matrix.shape[1],
        row_width // 2,
        rows,
    )
    x, g = input_activation_matrix[0], output_sensitivity[0]
    r, m, v = (
        array[0].reshape(rows, row_width)
        for array in (
            trajectory_initial_parameters,
            trajectory_gradient_average,
            trajectory_squared_average,
        )
    )
    common, inertia = common_expert_parameters, outer_inertia
    flags = punctual_flags
    scalars = (
        trajectory_membership,
        flags,
        lax.axis_index("path").astype(jnp.int32)[None],
    )
    shape = (1, set_count, local_units, row_width)

    def finish(arrived, rounds, j, partial):
        return finish_set(
            scalars, common, inertia, arrived, j, rounds, path_count, shape, partial
        )

    def both():
        (arrived,) = run_path(plan, False, flags, x, g, r, m, v)
        hops = list(range(path_count - 1, 0, -1))
        trade = {k: [(p, p ^ k) for p in range(path_count)] for k in hops}
        moved, partial = [], ()
        for j in range(owned_sets):
            *partial, = finish(arrived, 0, j, partial)
            blocks, partial = partial[3:], partial[:3]
            moved.append({k: lax.ppermute(blocks[k - 1], "path", trade[k]) for k in hops})
        experts, inertias, returned = partial
        for j in range(owned_sets):
            for k in reversed(hops):
                returned = place_block(scalars, returned, moved[j][k], j, owned_sets, k)
        return experts, inertias, returned

    cross = [(p, p ^ 2) for p in range(path_count)]
    swap = [(p, p ^ 1) for p in range(path_count)]

    def exchange(rounds, others, arrived, mine, early, needed):
        still = (early, lax.ppermute(early, "path", swap))
        moved, beside, rest, partial = [], [], [], ()
        for j in range(owned_sets):
            blocks = finish(arrived, rounds, j, partial)
            partial, (late_block, near_block, *other) = blocks[:3], blocks[3:]
            rest += other
            sent = lax.ppermute(late_block, "path", cross)
            moved.append((sent, lax.ppermute(sent, "path", swap)))
            beside.append(lax.ppermute(near_block, "path", swap))
        extra = [(None, None)] * owned_sets
        if others:
            if others < owned_sets:
                chosen = rest[-1]
                for j in range(owned_sets - 1):
                    chosen = jnp.where(needed[j], rest[j], chosen)
                rest = [chosen]
            sent = [lax.ppermute(block, "path", cross) for block in rest]
            sent = [(block, lax.ppermute(block, "path", swap)) for block in sent]
            extra = sent if others == owned_sets else sent * owned_sets
        experts, inertias, returned = partial
        for j in range(owned_sets):
            returned = place_block(scalars, returned, beside[j], j, owned_sets, 1)
        for j in range(owned_sets):
            for turn in range(2):
                returned = place_far(
                    scalars,
                    returned,
                    moved[j][turn],
                    still[turn],
                    mine,
                    extra[j][turn],
                    j,
                    owned_sets,
                    turn,
                )
        return experts, inertias, returned

    def survivors(rounds):
        base = pick_early(scalars, common, inertia)
        early = lax.ppermute(base, "path", cross)
        arrived, mine = run_survivors(plan, rounds, flags, x, g, r, m, v)
        if rounds == 1:
            return exchange(rounds, 0, arrived, mine, early, None)
        needed = []
        for chip in range(2):
            part = slice(chip * 2 * owned_sets, (chip + 1) * 2 * owned_sets)
            differ = trajectory_membership[0::2, part] != trajectory_membership[1::2, part]
            full = flags[2 * chip] + flags[2 * chip + 1] == 2
            needed.append(full & differ[0] & differ[1])
        needed = jnp.concatenate(needed).reshape(path_count, owned_sets)
        most = jnp.max(jnp.sum(needed.astype(jnp.int32), axis=1))
        own = needed[lax.axis_index("path")]
        return lax.switch(
            jnp.minimum(most, 2),
            [
                functools.partial(exchange, rounds, count)
                for count in (0, min(1, owned_sets), owned_sets)
            ],
            arrived,
            mine,
            early,
            own,
        )

    if path_count == 4 and choices == 2:
        lone = (flags[0] + flags[1] <= 1) & (flags[2] + flags[3] <= 1)
        return lax.cond(lone, lambda: survivors(1), lambda: survivors(2))
    return both()


def solution(mesh):
    placed = (
        P("path", "fsdp", None),
        P("path", "fsdp", None),
        P("path", None, "fsdp", None),
        P("path", None, "fsdp", None),
        P("path", None, "fsdp", None),
        P("path", None, "fsdp", None),
        P("path", None, "fsdp", None),
        P(),
        P(),
    )
    return jax.shard_map(
        per_device,
        mesh=mesh,
        in_specs=placed,
        out_specs=(
            P("path", None, "fsdp", None),
            P("path", None, "fsdp", None),
            P("path", None, "fsdp", None),
        ),
        check_vma=False,
    )
```

```python
import functools

import jax
import jax.numpy as jnp
from jax import lax
from jax.experimental import pallas as pl
from jax.experimental.pallas import tpu as pltpu
from jax.sharding import PartitionSpec as P


UNIT = 1024
SETS = 8
STEP = 1000


BETA_ONE = 0.9
BETA_TWO = 0.999
ADAM_EPS = 1e-08
INNER_RATE = 0.05
DECAY = 0.1
GLOBAL_LEARNING = 0.7
INERTIA_FACTOR = 0.9

MESH = pl.DeviceIdType.MESH
GELU_ROOT = 0.7978845608028654
GELU_CUBE = 0.044715


def adam_delta(grads, first, second, start):
    corr_one = 1.0 - BETA_ONE**STEP
    corr_two = 1.0 - BETA_TWO**STEP
    first_new = BETA_ONE * first.astype(jnp.float32) + (1.0 - BETA_ONE) * grads
    second_new = BETA_TWO * second.astype(jnp.float32) + (1.0 - BETA_TWO) * grads * grads
    direction = first_new / corr_one / (jnp.sqrt(second_new / corr_two) + ADAM_EPS)
    return (INNER_RATE * (direction + DECAY * start.astype(jnp.float32))).astype(jnp.bfloat16)


def adam_folded(product, scale, first, second, start):
    corr_one = 1.0 - BETA_ONE**STEP
    corr_two = 1.0 - BETA_TWO**STEP
    up = (BETA_ONE / corr_one) * first.astype(jnp.float32) + (
        (1.0 - BETA_ONE) / corr_one * scale
    ) * product
    spread = (BETA_TWO / corr_two) * second.astype(jnp.float32) + (
        (1.0 - BETA_TWO) / corr_two * scale * scale
    ) * (product * product)
    down = spread * lax.rsqrt(spread) + ADAM_EPS
    return (
        INNER_RATE * (up / down) + (INNER_RATE * DECAY) * start.astype(jnp.float32)
    ).astype(jnp.bfloat16)


def gelu_pair(pre):
    square = pre * pre
    tanh = jnp.tanh(GELU_ROOT * pre * (1.0 + GELU_CUBE * square))
    half = 0.5 * (1.0 + tanh)
    slope = half + 0.5 * pre * (1.0 - tanh * tanh) * GELU_ROOT * (1.0 + 3.0 * GELU_CUBE * square)
    return pre * half, slope


def divisor(total, wanted):
    size = min(total, wanted)
    while total % size:
        size //= 2
    return size


class Plan:
    def __init__(self, paths, ring, shard, features, rows):
        self.paths, self.ring, self.shard = paths, ring, shard
        self.features, self.width, self.rows = features, 2 * features, rows
        self.tokens = ring * shard
        self.half = shard // 2
        self.owned = rows // paths
        self.group = 1
        while (self.group * shard) % 128:
            self.group *= 2
        self.batch = self.group * shard
        self.tile = divisor(features, 512)
        self.tiles = self.width // self.tile
        self.units = divisor(rows, 256)
        self.pieces = 2 if self.half % 32 == 0 else 1
        self.slots = 3
        self.chunk = 256 if self.tokens % 256 == 0 else self.tokens


def ring_neighbours(index, size):
    odd = index % 2
    rank = (1 - odd) * (index // 2) + odd * (size - (index + 1) // 2)

    def place(r):
        high = r // (size // 2)
        return (1 - high) * 2 * r + high * (2 * (size - r) - 1)

    return place((rank + 1) % size), place((rank + size - 1) % size)


def path_kernel(
    plan, single, flags_ref, x_hbm, g_hbm, r_hbm, m_hbm, v_hbm, arr_hbm, own_hbm, *scratch
):
    (xg, params, hidden, first, second, pseudo) = scratch[:6]
    if single:
        (raw, swapped, cross_in, own_in, cross_out, own_out) = scratch[6:12]
    (load_sem, moment_sem, send_sem, recv_sem, side_send, side_recv, out_send, out_recv, keep_sem) = (
        scratch[-9:]
    )
    n, shard, half = plan.ring, plan.shard, plan.half
    features, owned, tile, tiles = plan.features, plan.owned, plan.tile, plan.tiles
    path = lax.axis_index("path")
    place = lax.axis_index("fsdp")
    ahead, behind = ring_neighbours(place, n)
    core = path % 2
    sibling = path + 1 - 2 * core
    lanes = 1 if single else 2

    barrier = pltpu.get_barrier_semaphore()
    for spot in (ahead, behind):
        pl.semaphore_signal(
            barrier, inc=1, device_id={"path": path, "fsdp": spot}, device_id_type=MESH
        )
    for k in range(1, plan.paths):
        pl.semaphore_signal(
            barrier,
            inc=1,
            device_id={"path": (path + k) % plan.paths, "fsdp": place},
            device_id_type=MESH,
        )

    def moments(t, slot):
        cols = pl.ds(pl.multiple_of(t * tile, tile), tile)
        return (
            pltpu.make_async_copy(m_hbm.at[:, cols], first.at[slot], moment_sem.at[0, slot]),
            pltpu.make_async_copy(v_hbm.at[:, cols], second.at[slot], moment_sem.at[1, slot]),
        )

    if single:
        loads = (
            pltpu.make_async_copy(x_hbm, raw.at[0], load_sem.at[0]),
            pltpu.make_async_copy(g_hbm, raw.at[1], load_sem.at[1]),
        )
    else:
        loads = (
            pltpu.make_async_copy(x_hbm, xg.at[0, pl.ds(0, shard)], load_sem.at[0]),
            pltpu.make_async_copy(g_hbm, xg.at[1, pl.ds(0, shard)], load_sem.at[1]),
        )
    for load in loads:
        load.start()
    load_params = pltpu.make_async_copy(r_hbm, params, load_sem.at[2])
    load_params.start()
    for load in moments(0, 0):
        load.start()
    pl.semaphore_wait(barrier, plan.paths + 1)
    for load in loads:
        load.wait()

    def ring_copy(step, lane, way):
        array = core if single else lane
        source = pl.ds(pl.multiple_of((step - 1) * shard + way * half, half), half)
        target = pl.ds(pl.multiple_of(step * shard + way * half, half), half)
        return pltpu.make_async_remote_copy(
            src_ref=xg.at[array, source],
            dst_ref=xg.at[array, target],
            send_sem=send_sem.at[lane, way, step],
            recv_sem=recv_sem.at[lane, way, step],
            device_id={"path": path, "fsdp": behind if way else ahead},
            device_id_type=MESH,
        )

    def side_copy(slot, array):
        rows = pl.ds(pl.multiple_of(slot * shard, shard), shard)
        return pltpu.make_async_remote_copy(
            src_ref=xg.at[array, rows],
            dst_ref=xg.at[array, rows],
            send_sem=side_send.at[slot],
            recv_sem=side_recv.at[slot],
            device_id={"path": sibling, "fsdp": place},
            device_id_type=MESH,
        )

    if single:
        active = lead_of(flags_ref, path // 2) == path
        swap = pltpu.make_async_remote_copy(
            src_ref=raw.at[1 - core],
            dst_ref=swapped,
            send_sem=load_sem.at[3],
            recv_sem=load_sem.at[4],
            device_id={"path": sibling, "fsdp": place},
            device_id_type=MESH,
        )
        swap.start()
        swap.wait()
        xg[core, 0:shard] = jnp.where(active, raw[core], swapped[...])

    load_params.wait()

    def forward(j):
        rows = pl.ds(pl.multiple_of(j * plan.batch, plan.batch), plan.batch)

        def unit(u, carry):
            strip = pl.ds(pl.multiple_of(u * plan.units, plan.units), plan.units)
            nt = (((1,), (1,)), ((), ()))
            pre = lax.dot_general(
                params[strip, 0:features], xg[0, rows], nt, preferred_element_type=jnp.float32
            ) * (features**-0.5)
            act, slope = gelu_pair(pre)
            hidden[1, strip, rows] = act.astype(jnp.bfloat16)
            back = lax.dot_general(
                params[strip, features : 2 * features],
                xg[1, rows],
                nt,
                preferred_element_type=jnp.float32,
            ) * ((SETS * UNIT) ** -0.5)
            hidden[0, strip, rows] = (back * slope).astype(jnp.bfloat16)
            return carry

        lax.fori_loop(0, plan.rows // plan.units, unit, 0)

    def gather_batch(j, carry):
        for i in range(plan.group):
            k = j * plan.group + i

            @pl.when(k > 0)
            def _():
                for lane in range(lanes):
                    for way in range(2):
                        ring_copy(k, lane, way).wait_recv()

            @pl.when(k < n - 1)
            def _():
                for lane in range(lanes):
                    for way in range(2):
                        ring_copy(k + 1, lane, way).start()

            if single:
                side_copy(k, core).start()
        if single:
            for i in range(plan.group):
                side_copy(j * plan.group + i, 1 - core).wait_recv()
        forward(j)
        return carry

    lax.fori_loop(0, n // plan.group, gather_batch, 0)

    def cols_of(t):
        return pl.ds(pl.multiple_of(t * tile, tile), tile)

    def rows_of(p):
        return pl.ds(pl.multiple_of(p * owned, owned), owned)

    chip = path // 2
    far = (1 - chip) * 2

    def out_copy(t, k):
        owner = (path + k) % plan.paths
        return pltpu.make_async_remote_copy(
            src_ref=pseudo.at[rows_of(owner), cols_of(t)],
            dst_ref=arr_hbm.at[path, :, cols_of(t)],
            send_sem=out_send.at[t, k],
            recv_sem=out_recv.at[t, k],
            device_id={"path": owner, "fsdp": place},
            device_id_type=MESH,
        )

    def keep_copy(t):
        return pltpu.make_async_copy(
            pseudo.at[rows_of(path), cols_of(t)],
            arr_hbm.at[path, :, cols_of(t)],
            keep_sem.at[0, t],
        )

    def share_copy(t, which):
        owner = (far + 1 - core) if which == 0 else sibling
        return pltpu.make_async_remote_copy(
            src_ref=pseudo.at[rows_of(owner), cols_of(t)],
            dst_ref=(cross_in if which == 0 else own_in).at[t],
            send_sem=out_send.at[t, which],
            recv_sem=out_recv.at[t, which],
            device_id={"path": sibling, "fsdp": place},
            device_id_type=MESH,
        )

    def cross_copy(t):
        return pltpu.make_async_remote_copy(
            src_ref=cross_out.at[t],
            dst_ref=arr_hbm.at[chip, :, cols_of(t)],
            send_sem=out_send.at[t, 2],
            recv_sem=out_recv.at[t, 2],
            device_id={"path": far + core, "fsdp": place},
            device_id_type=MESH,
        )

    def near_copy(t):
        return pltpu.make_async_copy(
            own_out.at[t], arr_hbm.at[chip, :, cols_of(t)], keep_sem.at[0, t]
        )

    def late_copy(t):
        return pltpu.make_async_copy(
            pseudo.at[pl.ds(pl.multiple_of(far * owned, 2 * owned), 2 * owned), cols_of(t)],
            own_hbm.at[:, cols_of(t)],
            keep_sem.at[1, t],
        )

    def pick(t):
        share_copy(t, 0).wait_recv()
        cross_out[t] = jnp.where(active, pseudo[rows_of(far + core), cols_of(t)], cross_in[t])
        cross_copy(t).start()
        share_copy(t, 1).wait_recv()
        own_out[t] = jnp.where(active, pseudo[rows_of(path), cols_of(t)], own_in[t])
        near_copy(t).start()

    def grad_tile(t, carry):
        slot = t % 2

        @pl.when(t + 1 < tiles)
        def _():
            for load in moments(t + 1, 1 - slot):
                load.start()

        for load in moments(t, slot):
            load.wait()
        side = t // (tiles // 2)
        scale = jnp.where(side == 0, features**-0.5, (SETS * UNIT) ** -0.5).astype(jnp.float32)
        token_cols = pl.ds(pl.multiple_of(t % (tiles // 2) * tile, tile), tile)

        def unit(u, inner):
            strip = pl.ds(pl.multiple_of(u * plan.units, plan.units), plan.units)
            grads = (
                jnp.dot(
                    hidden[side, strip, :],
                    xg[side, :, token_cols],
                    preferred_element_type=jnp.float32,
                )
                * scale
            )
            pseudo[strip, cols_of(t)] = adam_delta(
                grads, first[slot, strip, :], second[slot, strip, :], params[strip, cols_of(t)]
            )
            return inner

        lax.fori_loop(0, plan.rows // plan.units, unit, 0)
        if single:
            share_copy(t, 0).start()
            share_copy(t, 1).start()
            late_copy(t).start()

            @pl.when(t > 0)
            def _():
                pick(t - 1)
        else:
            for k in range(plan.paths - 1, 0, -1):
                out_copy(t, k).start()
            keep_copy(t).start()
        return carry

    lax.fori_loop(0, tiles, grad_tile, 0)
    if single:
        pick(tiles - 1)

    def drain_ring(k, carry):
        for lane in range(lanes):
            for way in range(2):
                ring_copy(k, lane, way).wait_send()
        return carry

    lax.fori_loop(1, n, drain_ring, 0)
    if single:

        def drain_side(k, carry):
            side_copy(k, core).wait_send()
            return carry

        lax.fori_loop(0, n, drain_side, 0)

    def drain(t, carry):
        if single:
            share_copy(t, 0).wait_send()
            share_copy(t, 1).wait_send()
            late_copy(t).wait()
            near_copy(t).wait()
            cross_copy(t).wait()
        else:
            for k in range(1, plan.paths):
                out_copy(t, k).wait()
            keep_copy(t).wait()
        return carry

    lax.fori_loop(0, tiles, drain, 0)


def run_path(plan, single, flags, x, g, r, m, v):
    bf16 = jnp.bfloat16
    width, tile, tiles = plan.width, plan.tile, plan.tiles
    scratch = [
        pltpu.VMEM((2, plan.tokens, plan.features), bf16),
        pltpu.VMEM((plan.rows, width), bf16),
        pltpu.VMEM((2, plan.rows, plan.tokens), bf16),
        pltpu.VMEM((2, plan.rows, tile), bf16),
        pltpu.VMEM((2, plan.rows, tile), bf16),
        pltpu.VMEM((plan.rows, width), bf16),
    ]
    if single:
        scratch += [
            pltpu.VMEM((2, plan.shard, plan.features), bf16),
            pltpu.VMEM((plan.shard, plan.features), bf16),
        ] + [pltpu.VMEM((tiles, plan.owned, tile), bf16)] * 4
    lanes = 1 if single else 2
    outs = 3 if single else plan.paths
    dma = pltpu.SemaphoreType.DMA
    scratch += [
        dma((5,)),
        dma((2, 2)),
        dma((lanes, 2, plan.ring)),
        dma((lanes, 2, plan.ring)),
        dma((plan.ring,)),
        dma((plan.ring,)),
        dma((tiles, outs)),
        dma((tiles, outs)),
        dma((2, tiles)),
    ]
    sources = 2 if single else plan.paths
    flops = 8 * plan.tokens * plan.features * plan.rows
    shapes = [jax.ShapeDtypeStruct((sources, plan.owned, width), bf16)]
    if single:
        shapes.append(jax.ShapeDtypeStruct((2 * plan.owned, width), bf16))
    body = functools.partial(path_kernel, plan, single)
    if not single:
        inner = body

        def body(flags_ref, x, g, r, m, v, arr, *rest):
            inner(flags_ref, x, g, r, m, v, arr, None, *rest)

    anywhere = pl.BlockSpec(memory_space=pl.ANY)
    return pl.pallas_call(
        body,
        out_shape=shapes,
        in_specs=[pl.BlockSpec(memory_space=pltpu.SMEM)] + [anywhere] * 5,
        out_specs=[anywhere] * len(shapes),
        scratch_shapes=scratch,
        compiler_params=pltpu.CompilerParams(
            collective_id=0 if single else 1,
            has_side_effects=True,
            vmem_limit_bytes=63 * 1024 * 1024,
        ),
        cost_estimate=pl.CostEstimate(
            flops=flops, bytes_accessed=8 * plan.rows * width, transcendentals=0
        ),
        name="single_path" if single else "both_paths",
    )(flags, x, g, r, m, v)


def survivor_kernel(
    plan,
    rounds,
    member_ref,
    flags_ref,
    x_hbm,
    g_hbm,
    r_hbm,
    m_hbm,
    v_hbm,
    common_hbm,
    inertia_hbm,
    arr_hbm,
    own_hbm,
    early_hbm,
    *scratch,
):
    (xg, params, hidden, first, second, pseudo, raw, swapped) = scratch[:8]
    (cross_in, own_in, cross_out, own_out, shown) = scratch[8:13]
    (load_sem, moment_sem, send_sem, recv_sem, side_send, side_recv, out_send, out_recv, keep_sem) = (
        scratch[13:22]
    )
    (shown_sem, early_sem) = scratch[22:]
    n, shard, half = plan.ring, plan.shard, plan.half
    features, owned, tile, tiles = plan.features, plan.owned, plan.tile, plan.tiles
    pieces, slots = plan.pieces, plan.slots
    path = lax.axis_index("path")
    place = lax.axis_index("fsdp")
    ahead, behind = ring_neighbours(place, n)
    core, chip = path % 2, path // 2
    sibling = path + 1 - 2 * core
    far = (1 - chip) * 2
    leading = jnp.where(lead_of(flags_ref, chip) == path, 1, 0)

    barrier = pltpu.get_barrier_semaphore()
    partners = [(path, ahead), (path, behind), (sibling, place), (far + core, place)]
    for to_path, to_place in partners:
        pl.semaphore_signal(
            barrier, inc=1, device_id={"path": to_path, "fsdp": to_place}, device_id_type=MESH
        )

    def cols_of(t):
        return pl.ds(pl.multiple_of(t * tile, tile), tile)

    def rows_of(p):
        return pl.ds(pl.multiple_of(p * owned, owned), owned)

    def moments(index):
        cols, slot = cols_of(index % tiles), index % 2
        return (
            pltpu.make_async_copy(m_hbm.at[:, cols], first.at[slot], moment_sem.at[0, slot]),
            pltpu.make_async_copy(v_hbm.at[:, cols], second.at[slot], moment_sem.at[1, slot]),
        )

    loads = (
        pltpu.make_async_copy(x_hbm, raw.at[0], load_sem.at[0]),
        pltpu.make_async_copy(g_hbm, raw.at[1], load_sem.at[1]),
    )
    for load in loads:
        load.start()
    load_params = pltpu.make_async_copy(r_hbm, params, load_sem.at[2])
    load_params.start()
    for load in moments(0):
        load.start()
    pl.semaphore_wait(barrier, len(partners))
    for load in loads:
        load.wait()
    swap = pltpu.make_async_remote_copy(
        src_ref=raw.at[1 - core],
        dst_ref=swapped,
        send_sem=load_sem.at[3],
        recv_sem=load_sem.at[4],
        device_id={"path": sibling, "fsdp": place},
        device_id_type=MESH,
    )
    swap.start()
    swap.wait()
    for turn in range(rounds):
        mine = leading == 1 - turn
        xg[turn, core, 0:shard] = jnp.where(mine, raw[core], swapped[...])

    def ring_copies(turn, step):
        copies = []
        for piece in range(pieces):
            for way in range(2):
                size = half // pieces
                at = way * half + piece * size
                source = pl.ds(pl.multiple_of((step - 1) * shard + at, 16), size)
                target = pl.ds(pl.multiple_of(step * shard + at, 16), size)
                copies.append(
                    pltpu.make_async_remote_copy(
                        src_ref=xg.at[turn, core, source],
                        dst_ref=xg.at[turn, core, target],
                        send_sem=send_sem.at[turn, way * pieces + piece, step],
                        recv_sem=recv_sem.at[turn, way * pieces + piece, step],
                        device_id={"path": path, "fsdp": behind if way else ahead},
                        device_id_type=MESH,
                    )
                )
        return copies

    def side_copy(turn, slot, array):
        rows = pl.ds(pl.multiple_of(slot * shard, shard), shard)
        return pltpu.make_async_remote_copy(
            src_ref=xg.at[turn, array, rows],
            dst_ref=xg.at[turn, array, rows],
            send_sem=side_send.at[turn, slot],
            recv_sem=side_recv.at[turn, slot],
            device_id={"path": sibling, "fsdp": place},
            device_id_type=MESH,
        )

    def show(e):
        return (
            pltpu.make_async_copy(
                common_hbm.at[:, :, :, cols_of(e)], shown.at[0], shown_sem.at[0]
            ),
            pltpu.make_async_copy(
                inertia_hbm.at[:, :, :, cols_of(e)], shown.at[1], shown_sem.at[1]
            ),
        )

    def early_copy(e):
        return pltpu.make_async_remote_copy(
            src_ref=cross_out.at[e],
            dst_ref=early_hbm.at[0, :, cols_of(e)],
            send_sem=early_sem.at[0, e],
            recv_sem=early_sem.at[1, e],
            device_id={"path": far + core, "fsdp": place},
            device_id_type=MESH,
        )

    def early_share(e):
        return pltpu.make_async_remote_copy(
            src_ref=early_hbm.at[0, :, cols_of(e)],
            dst_ref=early_hbm.at[1, :, cols_of(e)],
            send_sem=early_sem.at[2, e],
            recv_sem=early_sem.at[3, e],
            device_id={"path": sibling, "fsdp": place},
            device_id_type=MESH,
        )

    sets, units = shown.shape[1], shown.shape[3]

    def early_tile(e, carry):
        for load in show(e):
            load.wait()
        for j in range(sets):
            late = late_of(member_ref, flags_ref, path * sets + j, chip)
            common = jnp.where(late == 0, shown[0, j, 1], shown[0, j, 0])
            inertia = jnp.where(late == 0, shown[1, j, 1], shown[1, j, 0])
            base, _ = refreshed(0.0, 1.0, common, inertia)
            cross_out[e, j * units : (j + 1) * units] = base.astype(jnp.bfloat16)
        early_copy(e).start()

        @pl.when(e + 1 < tiles)
        def _():
            for load in show(e + 1):
                load.start()

        return carry

    for load in show(0):
        load.start()

    def begin(turn):
        for copy in ring_copies(turn, 1):
            copy.start()
        side_copy(turn, 0, core).start()

    begin(0)
    load_params.wait()

    def forward(turn, j):
        rows = pl.ds(pl.multiple_of(j * plan.chunk, plan.chunk), plan.chunk)

        def unit(u, carry):
            strip = pl.ds(pl.multiple_of(u * plan.units, plan.units), plan.units)
            nt = (((1,), (1,)), ((), ()))
            pre = lax.dot_general(
                params[strip, 0:features], xg[turn, 0, rows], nt, preferred_element_type=jnp.float32
            ) * (features**-0.5)
            act, slope = gelu_pair(pre)
            hidden[1, strip, rows] = act.astype(jnp.bfloat16)
            back = lax.dot_general(
                params[strip, features : 2 * features],
                xg[turn, 1, rows],
                nt,
                preferred_element_type=jnp.float32,
            ) * ((SETS * UNIT) ** -0.5)
            hidden[0, strip, rows] = (back * slope).astype(jnp.bfloat16)
            return carry

        lax.fori_loop(0, plan.rows // plan.units, unit, 0)

    def share_copy(index, which):
        owner = (far + 1 - core) if which == 0 else sibling
        return pltpu.make_async_remote_copy(
            src_ref=pseudo.at[index % slots, rows_of(owner)],
            dst_ref=(cross_in if which == 0 else own_in).at[index],
            send_sem=out_send.at[index, which],
            recv_sem=out_recv.at[index, which],
            device_id={"path": sibling, "fsdp": place},
            device_id_type=MESH,
        )

    def cross_copy(index):
        return pltpu.make_async_remote_copy(
            src_ref=cross_out.at[index % tiles],
            dst_ref=arr_hbm.at[index // tiles * 2 + chip, :, cols_of(index % tiles)],
            send_sem=out_send.at[index, 2],
            recv_sem=out_recv.at[index, 2],
            device_id={"path": far + core, "fsdp": place},
            device_id_type=MESH,
        )

    def near_copy(index):
        return pltpu.make_async_copy(
            own_out.at[index % tiles],
            arr_hbm.at[index // tiles * 2 + chip, :, cols_of(index % tiles)],
            keep_sem.at[0, index],
        )

    def own_copy(index):
        rows = pl.ds(pl.multiple_of(far * owned, 2 * owned), 2 * owned)
        out = pl.ds(pl.multiple_of(index // tiles * 2 * owned, 2 * owned), 2 * owned)
        return pltpu.make_async_copy(
            pseudo.at[index % slots, rows],
            own_hbm.at[out, cols_of(index % tiles)],
            keep_sem.at[1, index],
        )

    def pick(index):
        mine = leading == 1 - index // tiles

        @pl.when(index >= tiles)
        def _():
            cross_copy(index - tiles).wait_send()
            near_copy(index - tiles).wait()

        @pl.when(index < tiles)
        def _():
            early_copy(index).wait()
            early_share(index).start()

        slot, t = index % slots, index % tiles
        share_copy(index, 0).wait_recv()
        cross_out[t] = jnp.where(mine, pseudo[slot, rows_of(far + core)], cross_in[index])
        cross_copy(index).start()
        share_copy(index, 1).wait_recv()
        own_out[t] = jnp.where(mine, pseudo[slot, rows_of(path)], own_in[index])
        near_copy(index).start()

    def release(index):
        share_copy(index, 0).wait_send()
        share_copy(index, 1).wait_send()
        own_copy(index).wait()

    def grad_tile(index, carry):
        moment, slot = index % 2, index % slots
        turn, t = index // tiles, index % tiles

        @pl.when(index + 1 < rounds * tiles)
        def _():
            for load in moments(index + 1):
                load.start()

        @pl.when(index >= slots)
        def _():
            release(index - slots)

        for load in moments(index):
            load.wait()
        side = t // (tiles // 2)
        scale = jnp.where(side == 0, features**-0.5, (SETS * UNIT) ** -0.5).astype(jnp.float32)
        token_cols = pl.ds(pl.multiple_of(t % (tiles // 2) * tile, tile), tile)

        def unit(u, inner):
            strip = pl.ds(pl.multiple_of(u * plan.units, plan.units), plan.units)
            product = jnp.dot(
                hidden[side, strip, :],
                xg[turn, side, :, token_cols],
                preferred_element_type=jnp.float32,
            )
            pseudo[slot, strip, :] = adam_folded(
                product,
                scale,
                first[moment, strip, :],
                second[moment, strip, :],
                params[strip, cols_of(t)],
            )
            return inner

        lax.fori_loop(0, plan.rows // plan.units, unit, 0)
        share_copy(index, 0).start()
        share_copy(index, 1).start()
        own_copy(index).start()

        @pl.when(index > 0)
        def _():
            pick(index - 1)

        return carry

    spread = -(-tiles // 4)
    each = -(-tiles // n)
    last = rounds * n

    def stage(i, carry):
        turn, k = i // n, i % n

        @pl.when((k > 0) & (i < last))
        def _():
            arrivals = ring_copies(turn, k)

            @pl.when(k < n - 1)
            def _():
                for here, onward in zip(arrivals, ring_copies(turn, k + 1)):
                    here.wait_recv()
                    onward.start()

            @pl.when(k == n - 1)
            def _():
                for here in arrivals:
                    here.wait_recv()

            side_copy(turn, k, core).start()

        if rounds > 1:

            @pl.when((k == n - 1) & (turn + 1 < rounds))
            def _():
                begin(turn + 1)

        @pl.when(i < last)
        def _():
            side_copy(turn, k, 1 - core).wait_recv()

        begun, ended = k * shard // plan.chunk, (k + 1) * shard // plan.chunk
        if rounds == 1:
            low = jnp.where(i == last, 0, tiles)
            high = tiles
        else:
            held = (turn == 1) & (k < 4)
            low = jnp.where(held, k * spread, jnp.where(i == last, tiles, 0))
            high = jnp.where(
                held, jnp.minimum(k * spread + spread, tiles), jnp.where(i == last, 2 * tiles, 0)
            )
            begun = jnp.where((turn == 1) & (k < 6), jnp.where(k == 5, 2, 0), begun)
            ended = jnp.where((turn == 1) & (k < 5), jnp.where(k == 4, 2, 0), ended)
        lax.fori_loop(
            jnp.minimum(i * each, tiles), jnp.minimum((i + 1) * each, tiles), early_tile, 0
        )
        lax.fori_loop(low, high, grad_tile, 0)

        def ready(j, inner):
            forward(turn, j)
            return inner

        lax.fori_loop(jnp.where(i < last, begun, ended), ended, ready, 0)
        return carry

    lax.fori_loop(0, last + 1, stage, 0)
    pick(rounds * tiles - 1)

    def drain_ring(i, carry):
        turn, k = i // n, i % n
        side_copy(turn, k, core).wait_send()

        @pl.when(k > 0)
        def _():
            for copy in ring_copies(turn, k):
                copy.wait_send()

        return carry

    lax.fori_loop(0, rounds * n, drain_ring, 0)

    def drain(index, carry):
        @pl.when(index >= rounds * tiles - slots)
        def _():
            release(index)

        @pl.when(index >= (rounds - 1) * tiles)
        def _():
            near_copy(index).wait()
            cross_copy(index).wait_send()

        @pl.when(index < tiles)
        def _():
            early_share(index).wait()

        cross_copy(index).wait_recv()
        return carry

    lax.fori_loop(0, rounds * tiles, drain, 0)


def run_survivors(plan, rounds, member, flags, x, g, r, m, v, common, inertia):
    bf16, dma = jnp.bfloat16, pltpu.SemaphoreType.DMA
    width, tile, tiles = plan.width, plan.tile, plan.tiles
    served = pltpu.VMEM((rounds * tiles, plan.owned, tile), bf16)
    sent = pltpu.VMEM((tiles, plan.owned, tile), bf16)
    scratch = [
        pltpu.VMEM((rounds, 2, plan.tokens, plan.features), bf16),
        pltpu.VMEM((plan.rows, width), bf16),
        pltpu.VMEM((2, plan.rows, plan.tokens), bf16),
        pltpu.VMEM((2, plan.rows, tile), bf16),
        pltpu.VMEM((2, plan.rows, tile), bf16),
        pltpu.VMEM((plan.slots, plan.rows, tile), bf16),
        pltpu.VMEM((2, plan.shard, plan.features), bf16),
        pltpu.VMEM((plan.shard, plan.features), bf16),
        served,
        served,
        sent,
        sent,
        pltpu.VMEM((2,) + common.shape[:3] + (tile,), jnp.float32),
        dma((5,)),
        dma((2, 2)),
        dma((rounds, 2 * plan.pieces, plan.ring)),
        dma((rounds, 2 * plan.pieces, plan.ring)),
        dma((rounds, plan.ring)),
        dma((rounds, plan.ring)),
        dma((rounds * tiles, 3)),
        dma((rounds * tiles, 3)),
        dma((2, rounds * tiles)),
        dma((2,)),
        dma((4, tiles)),
    ]
    anywhere = pl.BlockSpec(memory_space=pl.ANY)
    return pl.pallas_call(
        functools.partial(survivor_kernel, plan, rounds),
        out_shape=[
            jax.ShapeDtypeStruct((2 * rounds, plan.owned, width), bf16),
            jax.ShapeDtypeStruct((2 * rounds * plan.owned, width), bf16),
            jax.ShapeDtypeStruct((2, plan.owned, width), bf16),
        ],
        in_specs=[pl.BlockSpec(memory_space=pltpu.SMEM)] * 2 + [anywhere] * 7,
        out_specs=[anywhere] * 3,
        scratch_shapes=scratch,
        compiler_params=pltpu.CompilerParams(
            collective_id=rounds, has_side_effects=True, vmem_limit_bytes=67043328
        ),
        cost_estimate=pl.CostEstimate(
            flops=8 * plan.tokens * plan.features * plan.rows * rounds,
            bytes_accessed=8 * plan.rows * width,
            transcendentals=0,
        ),
        name="survivors",
    )(member, flags, x, g, r, m, v, common, inertia)


def refreshed(total, tally, common, inertia):
    average = total / tally
    inertia = INERTIA_FACTOR * inertia + average
    expert = common - GLOBAL_LEARNING * (average + INERTIA_FACTOR * inertia)
    return expert, inertia


def lead_of(flags_ref, chip):
    return 2 * chip + jnp.where(flags_ref[2 * chip + 1] == 1, 1, 0)


def late_of(member_ref, flags_ref, at, owner_chip):
    far = 2 * (1 - owner_chip)
    near = member_ref[lead_of(flags_ref, owner_chip), at]
    shared = member_ref[far, at]
    return jnp.where(shared == member_ref[far + 1, at], shared, near)


def local_call(body, grid, in_specs, out_specs, out_shape, scalars, arrays, aliases=None):
    size = sum(array.size * array.dtype.itemsize for array in arrays)
    return pl.pallas_call(
        body,
        grid_spec=pltpu.PrefetchScalarGridSpec(
            num_scalar_prefetch=len(scalars), grid=grid, in_specs=in_specs, out_specs=out_specs
        ),
        out_shape=out_shape,
        input_output_aliases=aliases or {},
        compiler_params=pltpu.CompilerParams(vmem_limit_bytes=67043328),
        cost_estimate=pl.CostEstimate(flops=size, bytes_accessed=size, transcendentals=0),
    )(*scalars, *arrays)


ANYWHERE = pl.BlockSpec(memory_space=pl.ANY)


def finish_set(scalars, common, inertia, arrived, j, rounds, paths, shape, partial):
    sets, choices, units, width = common.shape
    sources = arrived.shape[0]
    step = divisor(width, 2048)
    sends = 1 + rounds if rounds else paths - 1

    def body(member_ref, flags_ref, spot_ref, shares, common_ref, inertia_ref, *refs):
        expert_out, inertia_out, returned, *outs = refs[-3 - sends :]
        spot = spot_ref[0]
        at = spot * sets + j
        updated = []
        for c in range(choices):
            total, count = 0.0, 0.0
            for p in range(paths):
                count += jnp.where((flags_ref[p] == 1) & (member_ref[p, at] == c), 1.0, 0.0)
            for q in range(sources):
                p = q
                if rounds:
                    lead = lead_of(flags_ref, q % 2)
                    p = lead if q < 2 else 4 * (q % 2) + 1 - lead
                weight = jnp.where((flags_ref[p] == 1) & (member_ref[p, at] == c), 1.0, 0.0)
                total = total + weight * shares[q].astype(jnp.float32)
            expert, moved = refreshed(
                total, jnp.maximum(count, 1.0), common_ref[0, c], inertia_ref[0, c]
            )
            expert_out[0, c] = expert
            inertia_out[0, c] = moved
            updated.append(expert.astype(jnp.bfloat16))

        def choose(index):
            chosen = updated[0]
            for c in range(1, choices):
                chosen = jnp.where(index == c, updated[c], chosen)
            return chosen

        returned[0, 0] = choose(member_ref[spot, at])
        if rounds:
            late = late_of(member_ref, flags_ref, at, spot // 2)
            outs[0][...] = choose(late)
            outs[1][...] = choose(member_ref[spot ^ 1, at])
            if rounds > 1:
                outs[2][...] = choose(1 - late)
        else:
            for k in range(1, paths):
                outs[k - 1][...] = choose(member_ref[spot ^ k, at])

    block = pl.BlockSpec((1, choices, units, step), lambda t, *_: (j, 0, 0, t))
    flat = pl.BlockSpec((units, step), lambda t, *_: (0, t))
    own = pl.BlockSpec((1, 1, units, step), lambda t, m, f, spot: (0, spot[0] * sets + j, 0, t))
    arrays = [arrived, common, inertia] + list(partial)
    return local_call(
        body,
        (width // step,),
        [pl.BlockSpec((sources, units, step), lambda t, *_: (0, j, t)), block, block]
        + [ANYWHERE] * len(partial),
        [block, block, own] + [flat] * sends,
        [jax.ShapeDtypeStruct(common.shape, jnp.float32)] * 2
        + [jax.ShapeDtypeStruct(shape, jnp.bfloat16)]
        + [jax.ShapeDtypeStruct((units, width), jnp.bfloat16)] * sends,
        scalars,
        arrays,
        {6 + i: i for i in range(len(partial))},
    )


def place_block(scalars, returned, block, j, sets, k):
    _, _, units, width = returned.shape
    step = divisor(width, 2048)

    def body(member_ref, flags_ref, spot_ref, block_ref, _, out):
        out[0, 0] = block_ref[...]

    return local_call(
        body,
        (width // step,),
        [pl.BlockSpec((units, step), lambda t, *_: (0, t)), ANYWHERE],
        pl.BlockSpec(
            (1, 1, units, step), lambda t, m, f, spot: (0, (spot[0] ^ k) * sets + j, 0, t)
        ),
        jax.ShapeDtypeStruct(returned.shape, jnp.bfloat16),
        scalars,
        [block, returned],
        {4: 0},
    )


def needs_other(member, flags, at, owner_chip):
    near, far = 2 * owner_chip, 2 * (1 - owner_chip)
    changed = (flags[near] == 1) & (flags[near + 1] == 1)
    changed &= member[near, at] != member[near + 1, at]
    return changed & (member[far, at] != member[far + 1, at])


def place_far(scalars, returned, late_block, early_block, mine, j, sets, turn):
    _, _, units, width = returned.shape
    step = divisor(width, 2048)

    def serving(spot):
        return (spot % 2) ^ turn

    def place(spot):
        return (2 * (1 - spot // 2) + serving(spot)) * sets + j

    def body(member_ref, flags_ref, spot_ref, late_ref, early_ref, mine_ref, *refs):
        out = refs[-1]
        spot = spot_ref[0]
        at = place(spot)
        gain = jnp.where(flags_ref[spot] == 1, GLOBAL_LEARNING * (1.0 + INERTIA_FACTOR), 0.0)
        late = late_of(member_ref, flags_ref, at, 1 - spot // 2)
        quiet = early_ref[0].astype(jnp.float32) - gain * mine_ref[...].astype(jnp.float32)
        quiet = quiet.astype(jnp.bfloat16)
        out[0, 0] = jnp.where(member_ref[spot, at] == late, late_ref[...], quiet)

    def mine_at(t, m, flags_ref, spot_ref):
        spot = spot_ref[0]
        behind = jnp.where(lead_of(flags_ref, spot // 2) == spot, 0, 1)
        turn_row = behind * (mine.shape[0] // units - 2 * sets)
        return (turn_row + serving(spot) * sets + j, t)

    flat = pl.BlockSpec((units, step), lambda t, *_: (0, t))
    arrays = [late_block, early_block, mine]
    specs = [
        flat,
        pl.BlockSpec((1, units, step), lambda t, *_: (turn, j, t)),
        pl.BlockSpec((units, step), mine_at),
    ]
    return local_call(
        body,
        (width // step,),
        specs + [ANYWHERE],
        pl.BlockSpec((1, 1, units, step), lambda t, m, f, spot: (0, place(spot[0]), 0, t)),
        jax.ShapeDtypeStruct(returned.shape, jnp.bfloat16),
        scalars,
        arrays + [returned],
        {3 + len(arrays): 0},
    )


def place_other(scalars, returned, block, j, sets, turn):
    _, _, units, width = returned.shape
    step = divisor(width, 2048)

    def place(member_ref, flags_ref, spot):
        first = (2 * (1 - spot // 2) + ((spot % 2) ^ turn)) * sets
        if j is not None:
            return first + j
        at = first + sets - 1
        for i in range(sets - 1):
            needed = needs_other(member_ref, flags_ref, first + i, 1 - spot // 2)
            at = jnp.where(needed, first + i, at)
        return at

    def body(member_ref, flags_ref, spot_ref, block_ref, before, out):
        spot = spot_ref[0]
        at = place(member_ref, flags_ref, spot)
        late = late_of(member_ref, flags_ref, at, 1 - spot // 2)
        sent = needs_other(member_ref, flags_ref, at, 1 - spot // 2)
        wanted = sent & (member_ref[spot, at] != late)
        out[0, 0] = jnp.where(wanted, block_ref[...], before[0, 0])

    spec = pl.BlockSpec(
        (1, 1, units, step), lambda t, m, f, spot_ref: (0, place(m, f, spot_ref[0]), 0, t)
    )
    return local_call(
        body,
        (width // step,),
        [pl.BlockSpec((units, step), lambda t, *_: (0, t)), spec],
        spec,
        jax.ShapeDtypeStruct(returned.shape, jnp.bfloat16),
        scalars,
        [block, returned],
        {4: 0},
    )


def per_device(
    input_activation_matrix,
    output_sensitivity,
    trajectory_initial_parameters,
    trajectory_gradient_average,
    trajectory_squared_average,
    common_expert_parameters,
    outer_inertia,
    trajectory_membership,
    punctual_flags,
):
    set_count, local_units, row_width = trajectory_initial_parameters.shape[1:]
    rows = set_count * local_units
    path_count = lax.axis_size("path")
    owned_sets = set_count // path_count
    choices = common_expert_parameters.shape[1]
    plan = Plan(
        path_count,
        lax.axis_size("fsdp"),
        input_activation_matrix.shape[1],
        row_width // 2,
        rows,
    )
    x, g = input_activation_matrix[0], output_sensitivity[0]
    r, m, v = (
        array[0].reshape(rows, row_width)
        for array in (
            trajectory_initial_parameters,
            trajectory_gradient_average,
            trajectory_squared_average,
        )
    )
    common, inertia = common_expert_parameters, outer_inertia
    flags = punctual_flags
    scalars = (
        trajectory_membership,
        flags,
        lax.axis_index("path").astype(jnp.int32)[None],
    )
    shape = (1, set_count, local_units, row_width)

    def finish(arrived, rounds, j, partial):
        return finish_set(
            scalars, common, inertia, arrived, j, rounds, path_count, shape, partial
        )

    def both():
        (arrived,) = run_path(plan, False, flags, x, g, r, m, v)
        hops = list(range(path_count - 1, 0, -1))
        trade = {k: [(p, p ^ k) for p in range(path_count)] for k in hops}
        moved, partial = [], ()
        for j in range(owned_sets):
            *partial, = finish(arrived, 0, j, partial)
            blocks, partial = partial[3:], partial[:3]
            moved.append({k: lax.ppermute(blocks[k - 1], "path", trade[k]) for k in hops})
        experts, inertias, returned = partial
        for j in range(owned_sets):
            for k in reversed(hops):
                returned = place_block(scalars, returned, moved[j][k], j, owned_sets, k)
        return experts, inertias, returned

    cross = [(p, p ^ 2) for p in range(path_count)]
    swap = [(p, p ^ 1) for p in range(path_count)]

    def exchange(rounds, others, arrived, mine, early, needed):
        moved, beside, rest, partial = [], [], [], ()
        for j in range(owned_sets):
            blocks = finish(arrived, rounds, j, partial)
            partial, (late_block, near_block, *other) = blocks[:3], blocks[3:]
            rest += other
            sent = lax.ppermute(late_block, "path", cross)
            moved.append((sent, lax.ppermute(sent, "path", swap)))
            beside.append(lax.ppermute(near_block, "path", swap))
        extra = []
        if others:
            if others < owned_sets:
                chosen = rest[-1]
                for j in range(owned_sets - 1):
                    chosen = jnp.where(needed[j], rest[j], chosen)
                rest = [chosen]
            sent = [lax.ppermute(block, "path", cross) for block in rest]
            extra = [(block, lax.ppermute(block, "path", swap)) for block in sent]
        experts, inertias, returned = partial
        for j in range(owned_sets):
            returned = place_block(scalars, returned, beside[j], j, owned_sets, 1)
        for j in range(owned_sets):
            for turn in range(2):
                returned = place_far(
                    scalars,
                    returned,
                    moved[j][turn],
                    early,
                    mine,
                    j,
                    owned_sets,
                    turn,
                )
        for j, pair in enumerate(extra):
            at = j if others == owned_sets else None
            for turn in range(2):
                returned = place_other(scalars, returned, pair[turn], at, owned_sets, turn)
        return experts, inertias, returned

    def survivors(rounds):
        arrived, mine, early = run_survivors(
            plan, rounds, trajectory_membership, flags, x, g, r, m, v, common, inertia
        )
        if rounds == 1:
            return exchange(rounds, 0, arrived, mine, early, None)
        pairs = trajectory_membership.reshape(2, 2, set_count)
        differ = (pairs[0, 0] != pairs[0, 1]) & (pairs[1, 0] != pairs[1, 1])
        alive = jnp.where(
            jnp.arange(set_count) < 2 * owned_sets, flags[0] + flags[1], flags[2] + flags[3]
        )
        needed = (differ & (alive == 2)).reshape(path_count, owned_sets)
        most = jnp.max(sum(needed[:, j].astype(jnp.int32) for j in range(owned_sets)))
        own = needed[lax.axis_index("path")]
        return lax.switch(
            jnp.minimum(most, 2),
            [
                functools.partial(exchange, rounds, count)
                for count in (0, min(1, owned_sets), owned_sets)
            ],
            arrived,
            mine,
            early,
            own,
        )

    if path_count == 4 and choices == 2:
        lone = (flags[0] + flags[1] <= 1) & (flags[2] + flags[3] <= 1)
        return lax.cond(lone, lambda: survivors(1), lambda: survivors(2))
    return both()


def solution(mesh):
    placed = (
        P("path", "fsdp", None),
        P("path", "fsdp", None),
        P("path", None, "fsdp", None),
        P("path", None, "fsdp", None),
        P("path", None, "fsdp", None),
        P("path", None, "fsdp", None),
        P("path", None, "fsdp", None),
        P(),
        P(),
    )
    return jax.shard_map(
        per_device,
        mesh=mesh,
        in_specs=placed,
        out_specs=(
            P("path", None, "fsdp", None),
            P("path", None, "fsdp", None),
            P("path", None, "fsdp", None),
        ),
        check_vma=False,
    )
```

```python
import functools

import jax
import jax.numpy as jnp
from jax import lax
from jax.experimental import pallas as pl
from jax.experimental.pallas import tpu as pltpu
from jax.sharding import PartitionSpec as P


UNIT = 1024
SETS = 8
STEP = 1000


BETA_ONE = 0.9
BETA_TWO = 0.999
ADAM_EPS = 1e-08
INNER_RATE = 0.05
DECAY = 0.1
GLOBAL_LEARNING = 0.7
INERTIA_FACTOR = 0.9

MESH = pl.DeviceIdType.MESH
GELU_ROOT = 0.7978845608028654
GELU_CUBE = 0.044715


def adam_delta(grads, first, second, start):
    corr_one = 1.0 - BETA_ONE**STEP
    corr_two = 1.0 - BETA_TWO**STEP
    first_new = BETA_ONE * first.astype(jnp.float32) + (1.0 - BETA_ONE) * grads
    second_new = BETA_TWO * second.astype(jnp.float32) + (1.0 - BETA_TWO) * grads * grads
    direction = first_new / corr_one / (jnp.sqrt(second_new / corr_two) + ADAM_EPS)
    return (INNER_RATE * (direction + DECAY * start.astype(jnp.float32))).astype(jnp.bfloat16)


def adam_folded(product, scale, first, second, start):
    corr_one = 1.0 - BETA_ONE**STEP
    corr_two = 1.0 - BETA_TWO**STEP
    up = (BETA_ONE / corr_one) * first.astype(jnp.float32) + (
        (1.0 - BETA_ONE) / corr_one * scale
    ) * product
    spread = (BETA_TWO / corr_two) * second.astype(jnp.float32) + (
        (1.0 - BETA_TWO) / corr_two * scale * scale
    ) * (product * product)
    down = spread * lax.rsqrt(spread) + ADAM_EPS
    return (
        INNER_RATE * (up / down) + (INNER_RATE * DECAY) * start.astype(jnp.float32)
    ).astype(jnp.bfloat16)


def gelu_pair(pre):
    square = pre * pre
    tanh = jnp.tanh(GELU_ROOT * pre * (1.0 + GELU_CUBE * square))
    half = 0.5 * (1.0 + tanh)
    slope = half + 0.5 * pre * (1.0 - tanh * tanh) * GELU_ROOT * (1.0 + 3.0 * GELU_CUBE * square)
    return pre * half, slope


def divisor(total, wanted):
    size = min(total, wanted)
    while total % size:
        size //= 2
    return size


class Plan:
    def __init__(self, paths, ring, shard, features, rows):
        self.paths, self.ring, self.shard = paths, ring, shard
        self.features, self.width, self.rows = features, 2 * features, rows
        self.tokens = ring * shard
        self.half = shard // 2
        self.owned = rows // paths
        self.group = 1
        while (self.group * shard) % 128:
            self.group *= 2
        self.batch = self.group * shard
        self.tile = divisor(features, 512)
        self.tiles = self.width // self.tile
        self.units = divisor(rows, 256)
        self.pieces = 2 if self.half % 32 == 0 else 1
        self.slots = 3
        self.chunk = 256 if self.tokens % 256 == 0 else self.tokens


def ring_neighbours(index, size):
    odd = index % 2
    rank = (1 - odd) * (index // 2) + odd * (size - (index + 1) // 2)

    def place(r):
        high = r // (size // 2)
        return (1 - high) * 2 * r + high * (2 * (size - r) - 1)

    return place((rank + 1) % size), place((rank + size - 1) % size)


def path_kernel(
    plan, single, flags_ref, x_hbm, g_hbm, r_hbm, m_hbm, v_hbm, arr_hbm, own_hbm, *scratch
):
    (xg, params, hidden, first, second, pseudo) = scratch[:6]
    if single:
        (raw, swapped, cross_in, own_in, cross_out, own_out) = scratch[6:12]
    (load_sem, moment_sem, send_sem, recv_sem, side_send, side_recv, out_send, out_recv, keep_sem) = (
        scratch[-9:]
    )
    n, shard, half = plan.ring, plan.shard, plan.half
    features, owned, tile, tiles = plan.features, plan.owned, plan.tile, plan.tiles
    path = lax.axis_index("path")
    place = lax.axis_index("fsdp")
    ahead, behind = ring_neighbours(place, n)
    core = path % 2
    sibling = path + 1 - 2 * core
    lanes = 1 if single else 2

    barrier = pltpu.get_barrier_semaphore()
    for spot in (ahead, behind):
        pl.semaphore_signal(
            barrier, inc=1, device_id={"path": path, "fsdp": spot}, device_id_type=MESH
        )
    for k in range(1, plan.paths):
        pl.semaphore_signal(
            barrier,
            inc=1,
            device_id={"path": (path + k) % plan.paths, "fsdp": place},
            device_id_type=MESH,
        )

    def moments(t, slot):
        cols = pl.ds(pl.multiple_of(t * tile, tile), tile)
        return (
            pltpu.make_async_copy(m_hbm.at[:, cols], first.at[slot], moment_sem.at[0, slot]),
            pltpu.make_async_copy(v_hbm.at[:, cols], second.at[slot], moment_sem.at[1, slot]),
        )

    if single:
        loads = (
            pltpu.make_async_copy(x_hbm, raw.at[0], load_sem.at[0]),
            pltpu.make_async_copy(g_hbm, raw.at[1], load_sem.at[1]),
        )
    else:
        loads = (
            pltpu.make_async_copy(x_hbm, xg.at[0, pl.ds(0, shard)], load_sem.at[0]),
            pltpu.make_async_copy(g_hbm, xg.at[1, pl.ds(0, shard)], load_sem.at[1]),
        )
    for load in loads:
        load.start()
    load_params = pltpu.make_async_copy(r_hbm, params, load_sem.at[2])
    load_params.start()
    for load in moments(0, 0):
        load.start()
    pl.semaphore_wait(barrier, plan.paths + 1)
    for load in loads:
        load.wait()

    def ring_copy(step, lane, way):
        array = core if single else lane
        source = pl.ds(pl.multiple_of((step - 1) * shard + way * half, half), half)
        target = pl.ds(pl.multiple_of(step * shard + way * half, half), half)
        return pltpu.make_async_remote_copy(
            src_ref=xg.at[array, source],
            dst_ref=xg.at[array, target],
            send_sem=send_sem.at[lane, way, step],
            recv_sem=recv_sem.at[lane, way, step],
            device_id={"path": path, "fsdp": behind if way else ahead},
            device_id_type=MESH,
        )

    def side_copy(slot, array):
        rows = pl.ds(pl.multiple_of(slot * shard, shard), shard)
        return pltpu.make_async_remote_copy(
            src_ref=xg.at[array, rows],
            dst_ref=xg.at[array, rows],
            send_sem=side_send.at[slot],
            recv_sem=side_recv.at[slot],
            device_id={"path": sibling, "fsdp": place},
            device_id_type=MESH,
        )

    if single:
        active = lead_of(flags_ref, path // 2) == path
        swap = pltpu.make_async_remote_copy(
            src_ref=raw.at[1 - core],
            dst_ref=swapped,
            send_sem=load_sem.at[3],
            recv_sem=load_sem.at[4],
            device_id={"path": sibling, "fsdp": place},
            device_id_type=MESH,
        )
        swap.start()
        swap.wait()
        xg[core, 0:shard] = jnp.where(active, raw[core], swapped[...])

    load_params.wait()

    def forward(j):
        rows = pl.ds(pl.multiple_of(j * plan.batch, plan.batch), plan.batch)

        def unit(u, carry):
            strip = pl.ds(pl.multiple_of(u * plan.units, plan.units), plan.units)
            nt = (((1,), (1,)), ((), ()))
            pre = lax.dot_general(
                params[strip, 0:features], xg[0, rows], nt, preferred_element_type=jnp.float32
            ) * (features**-0.5)
            act, slope = gelu_pair(pre)
            hidden[1, strip, rows] = act.astype(jnp.bfloat16)
            back = lax.dot_general(
                params[strip, features : 2 * features],
                xg[1, rows],
                nt,
                preferred_element_type=jnp.float32,
            ) * ((SETS * UNIT) ** -0.5)
            hidden[0, strip, rows] = (back * slope).astype(jnp.bfloat16)
            return carry

        lax.fori_loop(0, plan.rows // plan.units, unit, 0)

    def gather_batch(j, carry):
        for i in range(plan.group):
            k = j * plan.group + i

            @pl.when(k > 0)
            def _():
                for lane in range(lanes):
                    for way in range(2):
                        ring_copy(k, lane, way).wait_recv()

            @pl.when(k < n - 1)
            def _():
                for lane in range(lanes):
                    for way in range(2):
                        ring_copy(k + 1, lane, way).start()

            if single:
                side_copy(k, core).start()
        if single:
            for i in range(plan.group):
                side_copy(j * plan.group + i, 1 - core).wait_recv()
        forward(j)
        return carry

    lax.fori_loop(0, n // plan.group, gather_batch, 0)

    def cols_of(t):
        return pl.ds(pl.multiple_of(t * tile, tile), tile)

    def rows_of(p):
        return pl.ds(pl.multiple_of(p * owned, owned), owned)

    chip = path // 2
    far = (1 - chip) * 2

    def out_copy(t, k):
        owner = (path + k) % plan.paths
        return pltpu.make_async_remote_copy(
            src_ref=pseudo.at[rows_of(owner), cols_of(t)],
            dst_ref=arr_hbm.at[path, :, cols_of(t)],
            send_sem=out_send.at[t, k],
            recv_sem=out_recv.at[t, k],
            device_id={"path": owner, "fsdp": place},
            device_id_type=MESH,
        )

    def keep_copy(t):
        return pltpu.make_async_copy(
            pseudo.at[rows_of(path), cols_of(t)],
            arr_hbm.at[path, :, cols_of(t)],
            keep_sem.at[0, t],
        )

    def share_copy(t, which):
        owner = (far + 1 - core) if which == 0 else sibling
        return pltpu.make_async_remote_copy(
            src_ref=pseudo.at[rows_of(owner), cols_of(t)],
            dst_ref=(cross_in if which == 0 else own_in).at[t],
            send_sem=out_send.at[t, which],
            recv_sem=out_recv.at[t, which],
            device_id={"path": sibling, "fsdp": place},
            device_id_type=MESH,
        )

    def cross_copy(t):
        return pltpu.make_async_remote_copy(
            src_ref=cross_out.at[t],
            dst_ref=arr_hbm.at[chip, :, cols_of(t)],
            send_sem=out_send.at[t, 2],
            recv_sem=out_recv.at[t, 2],
            device_id={"path": far + core, "fsdp": place},
            device_id_type=MESH,
        )

    def near_copy(t):
        return pltpu.make_async_copy(
            own_out.at[t], arr_hbm.at[chip, :, cols_of(t)], keep_sem.at[0, t]
        )

    def late_copy(t):
        return pltpu.make_async_copy(
            pseudo.at[pl.ds(pl.multiple_of(far * owned, 2 * owned), 2 * owned), cols_of(t)],
            own_hbm.at[:, cols_of(t)],
            keep_sem.at[1, t],
        )

    def pick(t):
        share_copy(t, 0).wait_recv()
        cross_out[t] = jnp.where(active, pseudo[rows_of(far + core), cols_of(t)], cross_in[t])
        cross_copy(t).start()
        share_copy(t, 1).wait_recv()
        own_out[t] = jnp.where(active, pseudo[rows_of(path), cols_of(t)], own_in[t])
        near_copy(t).start()

    def grad_tile(t, carry):
        slot = t % 2

        @pl.when(t + 1 < tiles)
        def _():
            for load in moments(t + 1, 1 - slot):
                load.start()

        for load in moments(t, slot):
            load.wait()
        side = t // (tiles // 2)
        scale = jnp.where(side == 0, features**-0.5, (SETS * UNIT) ** -0.5).astype(jnp.float32)
        token_cols = pl.ds(pl.multiple_of(t % (tiles // 2) * tile, tile), tile)

        def unit(u, inner):
            strip = pl.ds(pl.multiple_of(u * plan.units, plan.units), plan.units)
            grads = (
                jnp.dot(
                    hidden[side, strip, :],
                    xg[side, :, token_cols],
                    preferred_element_type=jnp.float32,
                )
                * scale
            )
            pseudo[strip, cols_of(t)] = adam_delta(
                grads, first[slot, strip, :], second[slot, strip, :], params[strip, cols_of(t)]
            )
            return inner

        lax.fori_loop(0, plan.rows // plan.units, unit, 0)
        if single:
            share_copy(t, 0).start()
            share_copy(t, 1).start()
            late_copy(t).start()

            @pl.when(t > 0)
            def _():
                pick(t - 1)
        else:
            for k in range(plan.paths - 1, 0, -1):
                out_copy(t, k).start()
            keep_copy(t).start()
        return carry

    lax.fori_loop(0, tiles, grad_tile, 0)
    if single:
        pick(tiles - 1)

    def drain_ring(k, carry):
        for lane in range(lanes):
            for way in range(2):
                ring_copy(k, lane, way).wait_send()
        return carry

    lax.fori_loop(1, n, drain_ring, 0)
    if single:

        def drain_side(k, carry):
            side_copy(k, core).wait_send()
            return carry

        lax.fori_loop(0, n, drain_side, 0)

    def drain(t, carry):
        if single:
            share_copy(t, 0).wait_send()
            share_copy(t, 1).wait_send()
            late_copy(t).wait()
            near_copy(t).wait()
            cross_copy(t).wait()
        else:
            for k in range(1, plan.paths):
                out_copy(t, k).wait()
            keep_copy(t).wait()
        return carry

    lax.fori_loop(0, tiles, drain, 0)


def run_path(plan, single, flags, x, g, r, m, v):
    bf16 = jnp.bfloat16
    width, tile, tiles = plan.width, plan.tile, plan.tiles
    scratch = [
        pltpu.VMEM((2, plan.tokens, plan.features), bf16),
        pltpu.VMEM((plan.rows, width), bf16),
        pltpu.VMEM((2, plan.rows, plan.tokens), bf16),
        pltpu.VMEM((2, plan.rows, tile), bf16),
        pltpu.VMEM((2, plan.rows, tile), bf16),
        pltpu.VMEM((plan.rows, width), bf16),
    ]
    if single:
        scratch += [
            pltpu.VMEM((2, plan.shard, plan.features), bf16),
            pltpu.VMEM((plan.shard, plan.features), bf16),
        ] + [pltpu.VMEM((tiles, plan.owned, tile), bf16)] * 4
    lanes = 1 if single else 2
    outs = 3 if single else plan.paths
    dma = pltpu.SemaphoreType.DMA
    scratch += [
        dma((5,)),
        dma((2, 2)),
        dma((lanes, 2, plan.ring)),
        dma((lanes, 2, plan.ring)),
        dma((plan.ring,)),
        dma((plan.ring,)),
        dma((tiles, outs)),
        dma((tiles, outs)),
        dma((2, tiles)),
    ]
    sources = 2 if single else plan.paths
    flops = 8 * plan.tokens * plan.features * plan.rows
    shapes = [jax.ShapeDtypeStruct((sources, plan.owned, width), bf16)]
    if single:
        shapes.append(jax.ShapeDtypeStruct((2 * plan.owned, width), bf16))
    body = functools.partial(path_kernel, plan, single)
    if not single:
        inner = body

        def body(flags_ref, x, g, r, m, v, arr, *rest):
            inner(flags_ref, x, g, r, m, v, arr, None, *rest)

    anywhere = pl.BlockSpec(memory_space=pl.ANY)
    return pl.pallas_call(
        body,
        out_shape=shapes,
        in_specs=[pl.BlockSpec(memory_space=pltpu.SMEM)] + [anywhere] * 5,
        out_specs=[anywhere] * len(shapes),
        scratch_shapes=scratch,
        compiler_params=pltpu.CompilerParams(
            collective_id=0 if single else 1,
            has_side_effects=True,
            vmem_limit_bytes=63 * 1024 * 1024,
        ),
        cost_estimate=pl.CostEstimate(
            flops=flops, bytes_accessed=8 * plan.rows * width, transcendentals=0
        ),
        name="single_path" if single else "both_paths",
    )(flags, x, g, r, m, v)


def survivor_kernel(
    plan,
    rounds,
    member_ref,
    flags_ref,
    x_hbm,
    g_hbm,
    r_hbm,
    m_hbm,
    v_hbm,
    common_hbm,
    inertia_hbm,
    arr_hbm,
    own_hbm,
    early_hbm,
    *scratch,
):
    (xg, params, hidden, first, second, pseudo, raw, swapped) = scratch[:8]
    (cross_in, own_in, cross_out, own_out, shown) = scratch[8:13]
    (load_sem, moment_sem, send_sem, recv_sem, side_send, side_recv, out_send, out_recv, keep_sem) = (
        scratch[13:22]
    )
    (shown_sem, early_sem) = scratch[22:]
    n, shard, half = plan.ring, plan.shard, plan.half
    features, owned, tile, tiles = plan.features, plan.owned, plan.tile, plan.tiles
    pieces, slots = plan.pieces, plan.slots
    path = lax.axis_index("path")
    place = lax.axis_index("fsdp")
    ahead, behind = ring_neighbours(place, n)
    core, chip = path % 2, path // 2
    sibling = path + 1 - 2 * core
    far = (1 - chip) * 2
    leading = jnp.where(lead_of(flags_ref, chip) == path, 1, 0)

    barrier = pltpu.get_barrier_semaphore()
    partners = [(path, ahead), (path, behind), (sibling, place), (far + core, place)]
    for to_path, to_place in partners:
        pl.semaphore_signal(
            barrier, inc=1, device_id={"path": to_path, "fsdp": to_place}, device_id_type=MESH
        )

    def cols_of(t):
        return pl.ds(pl.multiple_of(t * tile, tile), tile)

    def rows_of(p):
        return pl.ds(pl.multiple_of(p * owned, owned), owned)

    def moments(index):
        cols, slot = cols_of(index % tiles), index % 2
        return (
            pltpu.make_async_copy(m_hbm.at[:, cols], first.at[slot], moment_sem.at[0, slot]),
            pltpu.make_async_copy(v_hbm.at[:, cols], second.at[slot], moment_sem.at[1, slot]),
        )

    loads = (
        pltpu.make_async_copy(x_hbm, raw.at[0], load_sem.at[0]),
        pltpu.make_async_copy(g_hbm, raw.at[1], load_sem.at[1]),
    )
    for load in loads:
        load.start()
    load_params = pltpu.make_async_copy(r_hbm, params, load_sem.at[2])
    load_params.start()
    for load in moments(0):
        load.start()
    pl.semaphore_wait(barrier, len(partners))
    for load in loads:
        load.wait()
    swap = pltpu.make_async_remote_copy(
        src_ref=raw.at[1 - core],
        dst_ref=swapped,
        send_sem=load_sem.at[3],
        recv_sem=load_sem.at[4],
        device_id={"path": sibling, "fsdp": place},
        device_id_type=MESH,
    )
    swap.start()
    swap.wait()
    for turn in range(rounds):
        mine = leading == 1 - turn
        xg[turn, core, 0:shard] = jnp.where(mine, raw[core], swapped[...])

    def ring_copies(turn, step):
        copies = []
        for piece in range(pieces):
            for way in range(2):
                size = half // pieces
                at = way * half + piece * size
                source = pl.ds(pl.multiple_of((step - 1) * shard + at, 16), size)
                target = pl.ds(pl.multiple_of(step * shard + at, 16), size)
                copies.append(
                    pltpu.make_async_remote_copy(
                        src_ref=xg.at[turn, core, source],
                        dst_ref=xg.at[turn, core, target],
                        send_sem=send_sem.at[turn, way * pieces + piece, step],
                        recv_sem=recv_sem.at[turn, way * pieces + piece, step],
                        device_id={"path": path, "fsdp": behind if way else ahead},
                        device_id_type=MESH,
                    )
                )
        return copies

    def side_copy(turn, slot, array):
        rows = pl.ds(pl.multiple_of(slot * shard, shard), shard)
        return pltpu.make_async_remote_copy(
            src_ref=xg.at[turn, array, rows],
            dst_ref=xg.at[turn, array, rows],
            send_sem=side_send.at[turn, slot],
            recv_sem=side_recv.at[turn, slot],
            device_id={"path": sibling, "fsdp": place},
            device_id_type=MESH,
        )

    def show(e):
        return (
            pltpu.make_async_copy(
                common_hbm.at[:, :, :, cols_of(e)], shown.at[0], shown_sem.at[0]
            ),
            pltpu.make_async_copy(
                inertia_hbm.at[:, :, :, cols_of(e)], shown.at[1], shown_sem.at[1]
            ),
        )

    def early_copy(e):
        return pltpu.make_async_remote_copy(
            src_ref=cross_out.at[e],
            dst_ref=early_hbm.at[0, :, cols_of(e)],
            send_sem=early_sem.at[0, e],
            recv_sem=early_sem.at[1, e],
            device_id={"path": far + core, "fsdp": place},
            device_id_type=MESH,
        )

    def early_share(e):
        return pltpu.make_async_remote_copy(
            src_ref=early_hbm.at[0, :, cols_of(e)],
            dst_ref=early_hbm.at[1, :, cols_of(e)],
            send_sem=early_sem.at[2, e],
            recv_sem=early_sem.at[3, e],
            device_id={"path": sibling, "fsdp": place},
            device_id_type=MESH,
        )

    sets, units = shown.shape[1], shown.shape[3]

    def early_tile(e, carry):
        for load in show(e):
            load.wait()
        for j in range(sets):
            late = late_of(member_ref, flags_ref, path * sets + j, chip)
            common = jnp.where(late == 0, shown[0, j, 1], shown[0, j, 0])
            inertia = jnp.where(late == 0, shown[1, j, 1], shown[1, j, 0])
            base, _ = refreshed(0.0, 1.0, common, inertia)
            cross_out[e, j * units : (j + 1) * units] = base.astype(jnp.bfloat16)
        early_copy(e).start()

        @pl.when(e + 1 < tiles)
        def _():
            for load in show(e + 1):
                load.start()

        return carry

    for load in show(0):
        load.start()

    def begin(turn):
        for copy in ring_copies(turn, 1):
            copy.start()
        side_copy(turn, 0, core).start()

    begin(0)
    load_params.wait()

    def forward(turn, j):
        rows = pl.ds(pl.multiple_of(j * plan.chunk, plan.chunk), plan.chunk)

        def unit(u, carry):
            strip = pl.ds(pl.multiple_of(u * plan.units, plan.units), plan.units)
            nt = (((1,), (1,)), ((), ()))
            pre = lax.dot_general(
                params[strip, 0:features], xg[turn, 0, rows], nt, preferred_element_type=jnp.float32
            ) * (features**-0.5)
            act, slope = gelu_pair(pre)
            hidden[1, strip, rows] = act.astype(jnp.bfloat16)
            back = lax.dot_general(
                params[strip, features : 2 * features],
                xg[turn, 1, rows],
                nt,
                preferred_element_type=jnp.float32,
            ) * ((SETS * UNIT) ** -0.5)
            hidden[0, strip, rows] = (back * slope).astype(jnp.bfloat16)
            return carry

        lax.fori_loop(0, plan.rows // plan.units, unit, 0)

    def share_copy(index, which):
        owner = (far + 1 - core) if which == 0 else sibling
        return pltpu.make_async_remote_copy(
            src_ref=pseudo.at[index % slots, rows_of(owner)],
            dst_ref=(cross_in if which == 0 else own_in).at[index],
            send_sem=out_send.at[index, which],
            recv_sem=out_recv.at[index, which],
            device_id={"path": sibling, "fsdp": place},
            device_id_type=MESH,
        )

    def cross_copy(index):
        return pltpu.make_async_remote_copy(
            src_ref=cross_out.at[index % tiles],
            dst_ref=arr_hbm.at[index // tiles * 2 + chip, :, cols_of(index % tiles)],
            send_sem=out_send.at[index, 2],
            recv_sem=out_recv.at[index, 2],
            device_id={"path": far + core, "fsdp": place},
            device_id_type=MESH,
        )

    def near_copy(index):
        return pltpu.make_async_copy(
            own_out.at[index % tiles],
            arr_hbm.at[index // tiles * 2 + chip, :, cols_of(index % tiles)],
            keep_sem.at[0, index],
        )

    def own_copy(index):
        rows = pl.ds(pl.multiple_of(far * owned, 2 * owned), 2 * owned)
        out = pl.ds(pl.multiple_of(index // tiles * 2 * owned, 2 * owned), 2 * owned)
        return pltpu.make_async_copy(
            pseudo.at[index % slots, rows],
            own_hbm.at[out, cols_of(index % tiles)],
            keep_sem.at[1, index],
        )

    def pick(index):
        mine = leading == 1 - index // tiles

        @pl.when(index >= tiles)
        def _():
            cross_copy(index - tiles).wait_send()
            near_copy(index - tiles).wait()

        @pl.when(index < tiles)
        def _():
            early_copy(index).wait()
            early_share(index).start()

        slot, t = index % slots, index % tiles
        share_copy(index, 0).wait_recv()
        cross_out[t] = jnp.where(mine, pseudo[slot, rows_of(far + core)], cross_in[index])
        cross_copy(index).start()
        share_copy(index, 1).wait_recv()
        own_out[t] = jnp.where(mine, pseudo[slot, rows_of(path)], own_in[index])
        near_copy(index).start()

    def release(index):
        share_copy(index, 0).wait_send()
        share_copy(index, 1).wait_send()
        own_copy(index).wait()

    def grad_tile(index, carry):
        moment, slot = index % 2, index % slots
        turn, t = index // tiles, index % tiles

        @pl.when(index + 1 < rounds * tiles)
        def _():
            for load in moments(index + 1):
                load.start()

        @pl.when(index >= slots)
        def _():
            release(index - slots)

        for load in moments(index):
            load.wait()
        side = t // (tiles // 2)
        scale = jnp.where(side == 0, features**-0.5, (SETS * UNIT) ** -0.5).astype(jnp.float32)
        token_cols = pl.ds(pl.multiple_of(t % (tiles // 2) * tile, tile), tile)

        def unit(u, inner):
            strip = pl.ds(pl.multiple_of(u * plan.units, plan.units), plan.units)
            product = jnp.dot(
                hidden[side, strip, :],
                xg[turn, side, :, token_cols],
                preferred_element_type=jnp.float32,
            )
            pseudo[slot, strip, :] = adam_folded(
                product,
                scale,
                first[moment, strip, :],
                second[moment, strip, :],
                params[strip, cols_of(t)],
            )
            return inner

        lax.fori_loop(0, plan.rows // plan.units, unit, 0)
        share_copy(index, 0).start()
        share_copy(index, 1).start()
        own_copy(index).start()

        @pl.when((index > 0) & (index % tiles != 1))
        def _():
            pick(index - 1)

        @pl.when(index % tiles == 0)
        def _():
            pick(index)

        return carry

    spread = -(-tiles // 4)
    each = -(-tiles // n)
    last = rounds * n

    def stage(i, carry):
        turn, k = i // n, i % n

        @pl.when((k > 0) & (i < last))
        def _():
            arrivals = ring_copies(turn, k)

            @pl.when(k < n - 1)
            def _():
                for here, onward in zip(arrivals, ring_copies(turn, k + 1)):
                    here.wait_recv()
                    onward.start()

            @pl.when(k == n - 1)
            def _():
                for here in arrivals:
                    here.wait_recv()

            side_copy(turn, k, core).start()

        if rounds > 1:

            @pl.when((k == n - 1) & (turn + 1 < rounds))
            def _():
                begin(turn + 1)

        @pl.when(i < last)
        def _():
            side_copy(turn, k, 1 - core).wait_recv()

        begun, ended = k * shard // plan.chunk, (k + 1) * shard // plan.chunk
        if rounds == 1:
            low = jnp.where(i == last, 0, tiles)
            high = tiles
        else:
            held = (turn == 1) & (k < 4)
            low = jnp.where(held, k * spread, jnp.where(i == last, tiles, 0))
            high = jnp.where(
                held, jnp.minimum(k * spread + spread, tiles), jnp.where(i == last, 2 * tiles, 0)
            )
            begun = jnp.where((turn == 1) & (k < 6), jnp.where(k == 5, 2, 0), begun)
            ended = jnp.where((turn == 1) & (k < 5), jnp.where(k == 4, 2, 0), ended)
        lax.fori_loop(
            jnp.minimum(i * each, tiles), jnp.minimum((i + 1) * each, tiles), early_tile, 0
        )
        lax.fori_loop(low, high, grad_tile, 0)

        def ready(j, inner):
            forward(turn, j)
            return inner

        lax.fori_loop(jnp.where(i < last, begun, ended), ended, ready, 0)
        return carry

    lax.fori_loop(0, last + 1, stage, 0)
    pick(rounds * tiles - 1)

    def drain_ring(i, carry):
        turn, k = i // n, i % n
        side_copy(turn, k, core).wait_send()

        @pl.when(k > 0)
        def _():
            for copy in ring_copies(turn, k):
                copy.wait_send()

        return carry

    lax.fori_loop(0, rounds * n, drain_ring, 0)

    def drain(index, carry):
        @pl.when(index >= rounds * tiles - slots)
        def _():
            release(index)

        @pl.when(index >= (rounds - 1) * tiles)
        def _():
            near_copy(index).wait()
            cross_copy(index).wait_send()

        @pl.when(index < tiles)
        def _():
            early_share(index).wait()

        cross_copy(index).wait_recv()
        return carry

    lax.fori_loop(0, rounds * tiles, drain, 0)


def run_survivors(plan, rounds, member, flags, x, g, r, m, v, common, inertia):
    bf16, dma = jnp.bfloat16, pltpu.SemaphoreType.DMA
    width, tile, tiles = plan.width, plan.tile, plan.tiles
    served = pltpu.VMEM((rounds * tiles, plan.owned, tile), bf16)
    sent = pltpu.VMEM((tiles, plan.owned, tile), bf16)
    scratch = [
        pltpu.VMEM((rounds, 2, plan.tokens, plan.features), bf16),
        pltpu.VMEM((plan.rows, width), bf16),
        pltpu.VMEM((2, plan.rows, plan.tokens), bf16),
        pltpu.VMEM((2, plan.rows, tile), bf16),
        pltpu.VMEM((2, plan.rows, tile), bf16),
        pltpu.VMEM((plan.slots, plan.rows, tile), bf16),
        pltpu.VMEM((2, plan.shard, plan.features), bf16),
        pltpu.VMEM((plan.shard, plan.features), bf16),
        served,
        served,
        sent,
        sent,
        pltpu.VMEM((2,) + common.shape[:3] + (tile,), jnp.float32),
        dma((5,)),
        dma((2, 2)),
        dma((rounds, 2 * plan.pieces, plan.ring)),
        dma((rounds, 2 * plan.pieces, plan.ring)),
        dma((rounds, plan.ring)),
        dma((rounds, plan.ring)),
        dma((rounds * tiles, 3)),
        dma((rounds * tiles, 3)),
        dma((2, rounds * tiles)),
        dma((2,)),
        dma((4, tiles)),
    ]
    anywhere = pl.BlockSpec(memory_space=pl.ANY)
    return pl.pallas_call(
        functools.partial(survivor_kernel, plan, rounds),
        out_shape=[
            jax.ShapeDtypeStruct((2 * rounds, plan.owned, width), bf16),
            jax.ShapeDtypeStruct((2 * rounds * plan.owned, width), bf16),
            jax.ShapeDtypeStruct((2, plan.owned, width), bf16),
        ],
        in_specs=[pl.BlockSpec(memory_space=pltpu.SMEM)] * 2 + [anywhere] * 7,
        out_specs=[anywhere] * 3,
        scratch_shapes=scratch,
        compiler_params=pltpu.CompilerParams(
            collective_id=rounds, has_side_effects=True, vmem_limit_bytes=67043328
        ),
        cost_estimate=pl.CostEstimate(
            flops=8 * plan.tokens * plan.features * plan.rows * rounds,
            bytes_accessed=8 * plan.rows * width,
            transcendentals=0,
        ),
        name="survivors",
    )(member, flags, x, g, r, m, v, common, inertia)


def refreshed(total, tally, common, inertia):
    average = total / tally
    inertia = INERTIA_FACTOR * inertia + average
    expert = common - GLOBAL_LEARNING * (average + INERTIA_FACTOR * inertia)
    return expert, inertia


def lead_of(flags_ref, chip):
    return 2 * chip + jnp.where(flags_ref[2 * chip + 1] == 1, 1, 0)


def late_of(member_ref, flags_ref, at, owner_chip):
    far = 2 * (1 - owner_chip)
    near = member_ref[lead_of(flags_ref, owner_chip), at]
    shared = member_ref[far, at]
    return jnp.where(shared == member_ref[far + 1, at], shared, near)


def local_call(body, grid, in_specs, out_specs, out_shape, scalars, arrays, aliases=None):
    size = sum(array.size * array.dtype.itemsize for array in arrays)
    return pl.pallas_call(
        body,
        grid_spec=pltpu.PrefetchScalarGridSpec(
            num_scalar_prefetch=len(scalars), grid=grid, in_specs=in_specs, out_specs=out_specs
        ),
        out_shape=out_shape,
        input_output_aliases=aliases or {},
        compiler_params=pltpu.CompilerParams(vmem_limit_bytes=67043328),
        cost_estimate=pl.CostEstimate(flops=size, bytes_accessed=size, transcendentals=0),
    )(*scalars, *arrays)


ANYWHERE = pl.BlockSpec(memory_space=pl.ANY)


def finish_set(scalars, common, inertia, arrived, j, rounds, paths, shape, partial):
    sets, choices, units, width = common.shape
    sources = arrived.shape[0]
    step = divisor(width, 2048)
    sends = 1 + rounds if rounds else paths - 1

    def body(member_ref, flags_ref, spot_ref, shares, common_ref, inertia_ref, *refs):
        expert_out, inertia_out, returned, *outs = refs[-3 - sends :]
        spot = spot_ref[0]
        at = spot * sets + j
        updated = []
        for c in range(choices):
            total, count = 0.0, 0.0
            for p in range(paths):
                count += jnp.where((flags_ref[p] == 1) & (member_ref[p, at] == c), 1.0, 0.0)
            for q in range(sources):
                p = q
                if rounds:
                    lead = lead_of(flags_ref, q % 2)
                    p = lead if q < 2 else 4 * (q % 2) + 1 - lead
                weight = jnp.where((flags_ref[p] == 1) & (member_ref[p, at] == c), 1.0, 0.0)
                total = total + weight * shares[q].astype(jnp.float32)
            expert, moved = refreshed(
                total, jnp.maximum(count, 1.0), common_ref[0, c], inertia_ref[0, c]
            )
            expert_out[0, c] = expert
            inertia_out[0, c] = moved
            updated.append(expert.astype(jnp.bfloat16))

        def choose(index):
            chosen = updated[0]
            for c in range(1, choices):
                chosen = jnp.where(index == c, updated[c], chosen)
            return chosen

        returned[0, 0] = choose(member_ref[spot, at])
        if rounds:
            late = late_of(member_ref, flags_ref, at, spot // 2)
            outs[0][...] = choose(late)
            outs[1][...] = choose(member_ref[spot ^ 1, at])
            if rounds > 1:
                outs[2][...] = choose(1 - late)
        else:
            for k in range(1, paths):
                outs[k - 1][...] = choose(member_ref[spot ^ k, at])

    block = pl.BlockSpec((1, choices, units, step), lambda t, *_: (j, 0, 0, t))
    flat = pl.BlockSpec((units, step), lambda t, *_: (0, t))
    own = pl.BlockSpec((1, 1, units, step), lambda t, m, f, spot: (0, spot[0] * sets + j, 0, t))
    arrays = [arrived, common, inertia] + list(partial)
    return local_call(
        body,
        (width // step,),
        [pl.BlockSpec((sources, units, step), lambda t, *_: (0, j, t)), block, block]
        + [ANYWHERE] * len(partial),
        [block, block, own] + [flat] * sends,
        [jax.ShapeDtypeStruct(common.shape, jnp.float32)] * 2
        + [jax.ShapeDtypeStruct(shape, jnp.bfloat16)]
        + [jax.ShapeDtypeStruct((units, width), jnp.bfloat16)] * sends,
        scalars,
        arrays,
        {6 + i: i for i in range(len(partial))},
    )


def place_block(scalars, returned, block, j, sets, k):
    _, _, units, width = returned.shape
    step = divisor(width, 2048)

    def body(member_ref, flags_ref, spot_ref, block_ref, _, out):
        out[0, 0] = block_ref[...]

    return local_call(
        body,
        (width // step,),
        [pl.BlockSpec((units, step), lambda t, *_: (0, t)), ANYWHERE],
        pl.BlockSpec(
            (1, 1, units, step), lambda t, m, f, spot: (0, (spot[0] ^ k) * sets + j, 0, t)
        ),
        jax.ShapeDtypeStruct(returned.shape, jnp.bfloat16),
        scalars,
        [block, returned],
        {4: 0},
    )


def needs_other(member, flags, at, owner_chip):
    near, far = 2 * owner_chip, 2 * (1 - owner_chip)
    changed = (flags[near] == 1) & (flags[near + 1] == 1)
    changed &= member[near, at] != member[near + 1, at]
    return changed & (member[far, at] != member[far + 1, at])


def place_far(scalars, returned, late_block, early_block, mine, j, sets, turn):
    _, _, units, width = returned.shape
    step = divisor(width, 2048)

    def serving(spot):
        return (spot % 2) ^ turn

    def place(spot):
        return (2 * (1 - spot // 2) + serving(spot)) * sets + j

    def body(member_ref, flags_ref, spot_ref, late_ref, early_ref, mine_ref, *refs):
        out = refs[-1]
        spot = spot_ref[0]
        at = place(spot)
        gain = jnp.where(flags_ref[spot] == 1, GLOBAL_LEARNING * (1.0 + INERTIA_FACTOR), 0.0)
        late = late_of(member_ref, flags_ref, at, 1 - spot // 2)
        quiet = early_ref[0].astype(jnp.float32) - gain * mine_ref[...].astype(jnp.float32)
        quiet = quiet.astype(jnp.bfloat16)
        out[0, 0] = jnp.where(member_ref[spot, at] == late, late_ref[...], quiet)

    def mine_at(t, m, flags_ref, spot_ref):
        spot = spot_ref[0]
        behind = jnp.where(lead_of(flags_ref, spot // 2) == spot, 0, 1)
        turn_row = behind * (mine.shape[0] // units - 2 * sets)
        return (turn_row + serving(spot) * sets + j, t)

    flat = pl.BlockSpec((units, step), lambda t, *_: (0, t))
    arrays = [late_block, early_block, mine]
    specs = [
        flat,
        pl.BlockSpec((1, units, step), lambda t, *_: (turn, j, t)),
        pl.BlockSpec((units, step), mine_at),
    ]
    return local_call(
        body,
        (width // step,),
        specs + [ANYWHERE],
        pl.BlockSpec((1, 1, units, step), lambda t, m, f, spot: (0, place(spot[0]), 0, t)),
        jax.ShapeDtypeStruct(returned.shape, jnp.bfloat16),
        scalars,
        arrays + [returned],
        {3 + len(arrays): 0},
    )


def place_other(scalars, returned, block, j, sets, turn):
    _, _, units, width = returned.shape
    step = divisor(width, 2048)

    def place(member_ref, flags_ref, spot):
        first = (2 * (1 - spot // 2) + ((spot % 2) ^ turn)) * sets
        if j is not None:
            return first + j
        at = first + sets - 1
        for i in range(sets - 1):
            needed = needs_other(member_ref, flags_ref, first + i, 1 - spot // 2)
            at = jnp.where(needed, first + i, at)
        return at

    def body(member_ref, flags_ref, spot_ref, block_ref, before, out):
        spot = spot_ref[0]
        at = place(member_ref, flags_ref, spot)
        late = late_of(member_ref, flags_ref, at, 1 - spot // 2)
        sent = needs_other(member_ref, flags_ref, at, 1 - spot // 2)
        wanted = sent & (member_ref[spot, at] != late)
        out[0, 0] = jnp.where(wanted, block_ref[...], before[0, 0])

    spec = pl.BlockSpec(
        (1, 1, units, step), lambda t, m, f, spot_ref: (0, place(m, f, spot_ref[0]), 0, t)
    )
    return local_call(
        body,
        (width // step,),
        [pl.BlockSpec((units, step), lambda t, *_: (0, t)), spec],
        spec,
        jax.ShapeDtypeStruct(returned.shape, jnp.bfloat16),
        scalars,
        [block, returned],
        {4: 0},
    )


def per_device(
    input_activation_matrix,
    output_sensitivity,
    trajectory_initial_parameters,
    trajectory_gradient_average,
    trajectory_squared_average,
    common_expert_parameters,
    outer_inertia,
    trajectory_membership,
    punctual_flags,
):
    set_count, local_units, row_width = trajectory_initial_parameters.shape[1:]
    rows = set_count * local_units
    path_count = lax.axis_size("path")
    owned_sets = set_count // path_count
    choices = common_expert_parameters.shape[1]
    plan = Plan(
        path_count,
        lax.axis_size("fsdp"),
        input_activation_matrix.shape[1],
        row_width // 2,
        rows,
    )
    x, g = input_activation_matrix[0], output_sensitivity[0]
    r, m, v = (
        array[0].reshape(rows, row_width)
        for array in (
            trajectory_initial_parameters,
            trajectory_gradient_average,
            trajectory_squared_average,
        )
    )
    common, inertia = common_expert_parameters, outer_inertia
    flags = punctual_flags
    scalars = (
        trajectory_membership,
        flags,
        lax.axis_index("path").astype(jnp.int32)[None],
    )
    shape = (1, set_count, local_units, row_width)

    def finish(arrived, rounds, j, partial):
        return finish_set(
            scalars, common, inertia, arrived, j, rounds, path_count, shape, partial
        )

    def both():
        (arrived,) = run_path(plan, False, flags, x, g, r, m, v)
        hops = list(range(path_count - 1, 0, -1))
        trade = {k: [(p, p ^ k) for p in range(path_count)] for k in hops}
        moved, partial = [], ()
        for j in range(owned_sets):
            *partial, = finish(arrived, 0, j, partial)
            blocks, partial = partial[3:], partial[:3]
            moved.append({k: lax.ppermute(blocks[k - 1], "path", trade[k]) for k in hops})
        experts, inertias, returned = partial
        for j in range(owned_sets):
            for k in reversed(hops):
                returned = place_block(scalars, returned, moved[j][k], j, owned_sets, k)
        return experts, inertias, returned

    cross = [(p, p ^ 2) for p in range(path_count)]
    swap = [(p, p ^ 1) for p in range(path_count)]

    def exchange(rounds, others, arrived, mine, early, needed):
        moved, beside, rest, partial = [], [], [], ()
        for j in range(owned_sets):
            blocks = finish(arrived, rounds, j, partial)
            partial, (late_block, near_block, *other) = blocks[:3], blocks[3:]
            rest += other
            sent = lax.ppermute(late_block, "path", cross)
            moved.append((sent, lax.ppermute(sent, "path", swap)))
            beside.append(lax.ppermute(near_block, "path", swap))
        extra = []
        if others:
            if others < owned_sets:
                chosen = rest[-1]
                for j in range(owned_sets - 1):
                    chosen = jnp.where(needed[j], rest[j], chosen)
                rest = [chosen]
            sent = [lax.ppermute(block, "path", cross) for block in rest]
            extra = [(block, lax.ppermute(block, "path", swap)) for block in sent]
        experts, inertias, returned = partial
        for j in range(owned_sets):
            returned = place_block(scalars, returned, beside[j], j, owned_sets, 1)
        for j in range(owned_sets):
            for turn in range(2):
                returned = place_far(
                    scalars,
                    returned,
                    moved[j][turn],
                    early,
                    mine,
                    j,
                    owned_sets,
                    turn,
                )
        for j, pair in enumerate(extra):
            at = j if others == owned_sets else None
            for turn in range(2):
                returned = place_other(scalars, returned, pair[turn], at, owned_sets, turn)
        return experts, inertias, returned

    def survivors(rounds):
        arrived, mine, early = run_survivors(
            plan, rounds, trajectory_membership, flags, x, g, r, m, v, common, inertia
        )
        if rounds == 1:
            return exchange(rounds, 0, arrived, mine, early, None)
        pairs = trajectory_membership.reshape(2, 2, set_count)
        differ = (pairs[0, 0] != pairs[0, 1]) & (pairs[1, 0] != pairs[1, 1])
        alive = jnp.where(
            jnp.arange(set_count) < 2 * owned_sets, flags[0] + flags[1], flags[2] + flags[3]
        )
        needed = (differ & (alive == 2)).reshape(path_count, owned_sets)
        most = jnp.max(sum(needed[:, j].astype(jnp.int32) for j in range(owned_sets)))
        own = needed[lax.axis_index("path")]
        return lax.switch(
            jnp.minimum(most, 2),
            [
                functools.partial(exchange, rounds, count)
                for count in (0, min(1, owned_sets), owned_sets)
            ],
            arrived,
            mine,
            early,
            own,
        )

    if path_count == 4 and choices == 2:
        lone = (flags[0] + flags[1] <= 1) & (flags[2] + flags[3] <= 1)
        return lax.cond(lone, lambda: survivors(1), lambda: survivors(2))
    return both()


def solution(mesh):
    placed = (
        P("path", "fsdp", None),
        P("path", "fsdp", None),
        P("path", None, "fsdp", None),
        P("path", None, "fsdp", None),
        P("path", None, "fsdp", None),
        P("path", None, "fsdp", None),
        P("path", None, "fsdp", None),
        P(),
        P(),
    )
    return jax.shard_map(
        per_device,
        mesh=mesh,
        in_specs=placed,
        out_specs=(
            P("path", None, "fsdp", None),
            P("path", None, "fsdp", None),
            P("path", None, "fsdp", None),
        ),
        check_vma=False,
    )
```
